32 devices in a mesh: dp: 8 (over y, x, core), seq: 4 (over z).
Axes of the slice: x: 2, y: 2, z: 4, core: 2. Of those that a mesh axis runs over, the one named last changes fastest.
Arguments:
- images: bfloat16 [16, 1152, 1024], P('dp', 'seq'), may hold values from -6 to 6
- qkv_weight: bfloat16 [1024, 3072], P('dp'), may hold values from -4 to 4, as said below
- qv_bias: bfloat16 [2048], P('dp'), may hold values from -3 to 3
- proj_weight: bfloat16 [1024, 1024], P('dp'), may hold values from -3.5 to 3.5
- proj_bias: bfloat16 [1024], P('dp'), may hold values from -3 to 3
- ln1_gain: bfloat16 [1024], P('dp'), may hold values from 0.25 to 1.75
- ln1_bias: bfloat16 [1024], P('dp'), may hold values from -3 to 3
- ln2_gain: bfloat16 [1024], P('dp'), may hold values from 0.25 to 1.75
- ln2_bias: bfloat16 [1024], P('dp'), may hold values from -3 to 3
- fc1_weight: bfloat16 [1024, 4096], P('dp'), may hold values from -0.1875 to 0.1875
- fc1_bias: bfloat16 [4096], P('dp'), may hold values from -3 to 3
- fc2_weight: bfloat16 [4096, 1024], P('dp'), may hold values from -0.09375 to 0.09375
- fc2_bias: bfloat16 [1024], P('dp'), may hold values from -3 to 3
- cotangent: bfloat16 [16, 1152, 1024], P('dp', 'seq'), may hold values from -6 to 6
Outputs:
- output: float32 [16, 1152, 1024], P('dp', 'seq')
- image_grad: float32 [16, 1152, 1024], P('dp', 'seq')
- qkv_weight_grad: float32 [1024, 3072], P('dp')
- qv_bias_grad: float32 [2048], P('dp')
- proj_weight_grad: float32 [1024, 1024], P('dp')
- proj_bias_grad: float32 [1024], P('dp')
- ln1_gain_grad: float32 [1024], P('dp')
- ln1_bias_grad: float32 [1024], P('dp')
- ln2_gain_grad: float32 [1024], P('dp')
- ln2_bias_grad: float32 [1024], P('dp')
- fc1_weight_grad: float32 [1024, 4096], P('dp')
- fc1_bias_grad: float32 [4096], P('dp')
- fc2_weight_grad: float32 [4096, 1024], P('dp')
- fc2_bias_grad: float32 [1024], P('dp')
The draws below stay inside these ranges and needn't reach their ends.
Inputs may be any that keep to these rules, and one draw needn't show every extreme that they name: `qkv_weight`: most entries are of order 1024^-1/2; others may be larger, within the stated range.
All inputs are finite; a program needn't handle non-finite values.
Results may differ from the reference program's by a relative error of at most 0.02.
The reference program's roundings to bfloat16 on the way count: a program that leaves them out, or rounds other values in their place, can miss the bound.
Values may be sent and summed in bfloat16 or wider, within the bound.
A program may use at most 256 MiB of HBM per device.

```python
import jax
import jax.numpy as jnp
from jax import lax

D = 1024
HEADS = 16
HEAD_DIM = 64
FF = 4096
SEQ_LEN = 1152
IMAGES = 16


def draw_qkv_weight(key, part):
    base_key = jax.random.fold_in(jax.random.fold_in(key, 7), 0)
    entries = jnp.clip(jax.random.normal(base_key, (D, 3 * D), jnp.float32), -4.0, 4.0) * D ** (-0.5)
    return entries.astype(jnp.bfloat16)


def levels(rng, extent, shards, low, top_value):
    level = 1.0
    for dim, parts in shards:
        steps = jax.random.uniform(jax.random.fold_in(jax.random.fold_in(rng, 6), dim), (parts,), jnp.float32, low / len(shards), top_value / len(shards))
        level = level * jnp.repeat(jnp.exp(steps), extent[dim] // parts).reshape((-1,) + (1,) * (len(extent) - 1 - dim))
    return level


def scatter_about(stream_key, shape, spread, most, shards=(), kind=jnp.bfloat16):
    level = levels(stream_key, shape, shards, -0.22, 0.18) if shards else 1.0
    drawn = jax.random.normal(stream_key, shape, jnp.float32) * spread * level
    return jnp.minimum(jnp.maximum(drawn, -most), most).astype(kind)


def setup_inputs(seed: int = 0) -> dict:
    keys = jax.random.split(jax.random.key(seed), 15)
    return {
        "images": scatter_about(keys[0], (IMAGES, SEQ_LEN, D), 1.0, 6.0, ((0, 8), (1, 4))),
        "qkv_weight": draw_qkv_weight(jax.random.fold_in(keys[14], 71), 0),
        "qv_bias": scatter_about(keys[2], (2 * D,), 0.5, 3.0, ((0, 8),)),
        "proj_weight": scatter_about(keys[3], (D, D), (max(1, 4 * D // SEQ_LEN)) ** -0.5, 3.5, ((0, 8),)),
        "proj_bias": scatter_about(keys[4], (D,), 0.5, 3.0, ((0, 8),)),
        "ln1_gain": jnp.clip(1.0 + 0.15 * jax.random.normal(keys[5], (D,), jnp.float32), 0.25, 1.75).astype(jnp.bfloat16),
        "ln1_bias": scatter_about(keys[6], (D,), 0.5, 3.0, ((0, 8),)),
        "ln2_gain": jnp.clip(1.0 + 0.15 * jax.random.normal(keys[7], (D,), jnp.float32), 0.25, 1.75).astype(jnp.bfloat16),
        "ln2_bias": scatter_about(keys[8], (D,), 0.5, 3.0, ((0, 8),)),
        "fc1_weight": scatter_about(keys[9], (D, FF), D ** -0.5, 0.1875, ((0, 8),)),
        "fc1_bias": scatter_about(keys[10], (FF,), 0.5, 3.0, ((0, 8),)),
        "fc2_weight": scatter_about(keys[11], (FF, D), FF ** -0.5, 0.09375, ((0, 8),)),
        "fc2_bias": scatter_about(keys[12], (D,), 0.5, 3.0, ((0, 8),)),
        "cotangent": scatter_about(keys[13], (IMAGES, SEQ_LEN, D), 1.0, 6.0, ((0, 8), (1, 4))),
    }


epsilon = 1e-06

def lowered(values):
    return lax.optimization_barrier(values.astype(jnp.bfloat16)).astype(jnp.float32)

def norm_forward(matrix, gain, shift):
    mean_val = lax.optimization_barrier(jnp.mean(matrix, axis=-1, keepdims=True))
    centred = matrix - mean_val
    inv_std = lax.rsqrt(lax.optimization_barrier(jnp.mean(centred * centred, axis=-1, keepdims=True)) + epsilon)
    normed = centred * inv_std
    return (normed, inv_std, normed * gain + shift)

def norm_backward(grad_in, normed, inv_std, gain):
    scaled = grad_in * gain
    return inv_std * (scaled - lax.optimization_barrier(jnp.mean(scaled, axis=-1, keepdims=True)) - normed * lax.optimization_barrier(jnp.mean(scaled * normed, axis=-1, keepdims=True)))

def gelu_cdf(pre_act):
    return 0.5 * (1.0 + lax.erf(pre_act * 0.7071067811865476))

def gelu_slope(pre_act):
    return gelu_cdf(pre_act) + pre_act * jnp.exp(-0.5 * pre_act * pre_act) * 0.3989422804014327

def reference(images, qkv_weight, qv_bias, proj_weight, proj_bias, ln1_gain, ln1_bias, ln2_gain, ln2_bias, fc1_weight, fc1_bias, fc2_weight, fc2_bias, cotangent):
    score_scale = HEAD_DIM ** (-0.5)
    gain_first = ln1_gain.astype(jnp.float32)
    shift_first = ln1_bias.astype(jnp.float32)
    gain_second = ln2_gain.astype(jnp.float32)
    shift_second = ln2_bias.astype(jnp.float32)
    bias_proj = proj_bias.astype(jnp.float32)
    bias_hidden = fc1_bias.astype(jnp.float32)
    bias_out = fc2_bias.astype(jnp.float32)
    bias_row = jnp.concatenate([qv_bias[:D].astype(jnp.float32), jnp.zeros((D,), jnp.float32), qv_bias[D:].astype(jnp.float32)])

    def split_heads(matrix):
        return matrix.reshape(SEQ_LEN, HEADS, HEAD_DIM).transpose(1, 0, 2)

    def join_heads(stacked):
        return stacked.transpose(1, 0, 2).reshape(SEQ_LEN, D)

    def head_forward(pieces):
        query_rows, key_rows, value_rows = pieces
        scores = jnp.dot(query_rows.astype(jnp.float32), key_rows.astype(jnp.float32).T) * score_scale
        row_peak = lax.optimization_barrier(jnp.max(scores, axis=-1, keepdims=True))
        lifted = jnp.exp(scores - row_peak)
        row_total = lax.optimization_barrier(jnp.sum(lifted, axis=-1, keepdims=True))
        probs_low = lowered(lifted / row_total)
        attended = jnp.dot(probs_low, value_rows.astype(jnp.float32)).astype(jnp.bfloat16)
        return (attended, (row_peak + jnp.log(row_total))[:, 0])

    def head_backward(pieces):
        query_rows, key_rows, value_rows, attended, grad_rows, log_total = pieces
        query_wide = query_rows.astype(jnp.float32)
        key_wide = key_rows.astype(jnp.float32)
        grad_wide = grad_rows.astype(jnp.float32)
        scores = jnp.dot(query_wide, key_wide.T) * score_scale
        probs = jnp.exp(scores - log_total[:, None])
        value_grad = jnp.dot(lowered(probs).T, grad_wide)
        prob_grad = jnp.dot(grad_wide, value_rows.astype(jnp.float32).T)
        delta_rows = lax.optimization_barrier(jnp.sum(grad_wide * attended.astype(jnp.float32), axis=-1, keepdims=True))
        score_grad = lowered(probs * (prob_grad - delta_rows) * score_scale)
        query_grad = jnp.dot(score_grad, key_wide)
        key_grad = jnp.dot(score_grad.T, query_wide)
        return (query_grad, key_grad, value_grad)

    def one_image(totals, inputs):
        image_rows, grad_low = inputs
        flat_rows = image_rows.astype(jnp.float32)
        normed_first, inv_first, pre_first = norm_forward(flat_rows, gain_first, shift_first)
        hidden_first = pre_first.astype(jnp.bfloat16)
        projected = (jnp.dot(hidden_first, qkv_weight, preferred_element_type=jnp.float32) + bias_row).astype(jnp.bfloat16)
        query_heads = split_heads(projected[:, :D])
        key_heads = split_heads(projected[:, D:2 * D])
        value_heads = split_heads(projected[:, 2 * D:])
        attended, log_total = lax.map(head_forward, (query_heads, key_heads, value_heads))
        attended_rows = join_heads(attended)
        residual_first = flat_rows + jnp.dot(attended_rows, proj_weight, preferred_element_type=jnp.float32) + bias_proj
        normed_second, inv_second, pre_second = norm_forward(residual_first, gain_second, shift_second)
        hidden_second = pre_second.astype(jnp.bfloat16)
        pre_act = jnp.dot(hidden_second, fc1_weight, preferred_element_type=jnp.float32) + bias_hidden
        acts = (pre_act * gelu_cdf(pre_act)).astype(jnp.bfloat16)
        output = residual_first + jnp.dot(acts, fc2_weight, preferred_element_type=jnp.float32) + bias_out
        grad_out = grad_low.astype(jnp.float32)
        grad_fc_two = jnp.dot(acts.T, grad_low, preferred_element_type=jnp.float32)
        grad_bias_two = lax.optimization_barrier(jnp.sum(grad_out, axis=0))
        pre_grad = jnp.dot(grad_low, fc2_weight.T, preferred_element_type=jnp.float32) * gelu_slope(pre_act)
        pre_grad_low = pre_grad.astype(jnp.bfloat16)
        grad_fc_one = jnp.dot(hidden_second.T, pre_grad_low, preferred_element_type=jnp.float32)
        grad_bias_one = lax.optimization_barrier(jnp.sum(pre_grad, axis=0))
        hidden_second_grad = jnp.dot(pre_grad_low, fc1_weight.T, preferred_element_type=jnp.float32)
        grad_gain_second = lax.optimization_barrier(jnp.sum(hidden_second_grad * normed_second, axis=0))
        grad_shift_second = lax.optimization_barrier(jnp.sum(hidden_second_grad, axis=0))
        residual_grad = grad_out + norm_backward(hidden_second_grad, normed_second, inv_second, gain_second)
        residual_grad_low = residual_grad.astype(jnp.bfloat16)
        grad_proj = jnp.dot(attended_rows.T, residual_grad_low, preferred_element_type=jnp.float32)
        grad_proj_bias = lax.optimization_barrier(jnp.sum(residual_grad, axis=0))
        attended_grad = jnp.dot(residual_grad_low, proj_weight.T, preferred_element_type=jnp.float32).astype(jnp.bfloat16)
        query_grad, key_grad, value_grad = lax.map(head_backward, (query_heads, key_heads, value_heads, attended, split_heads(attended_grad), log_total))
        query_rows_grad = join_heads(query_grad)
        value_rows_grad = join_heads(value_grad)
        grad_qv = jnp.concatenate([lax.optimization_barrier(jnp.sum(query_rows_grad, axis=0)), lax.optimization_barrier(jnp.sum(value_rows_grad, axis=0))])
        qkv_grad = jnp.concatenate([query_rows_grad, join_heads(key_grad), value_rows_grad], axis=1).astype(jnp.bfloat16)
        grad_qkv = jnp.dot(hidden_first.T, qkv_grad, preferred_element_type=jnp.float32)
        hidden_first_grad = jnp.dot(qkv_grad, qkv_weight.T, preferred_element_type=jnp.float32)
        grad_gain_first = lax.optimization_barrier(jnp.sum(hidden_first_grad * normed_first, axis=0))
        grad_shift_first = lax.optimization_barrier(jnp.sum(hidden_first_grad, axis=0))
        image_grad = residual_grad + norm_backward(hidden_first_grad, normed_first, inv_first, gain_first)
        grad_terms = (grad_qkv, grad_qv, grad_proj, grad_proj_bias, grad_gain_first, grad_shift_first, grad_gain_second, grad_shift_second, grad_fc_one, grad_bias_one, grad_fc_two, grad_bias_two)
        totals = jax.tree.map(lambda left, right: left + right, totals, grad_terms)
        return (totals, (output, image_grad))
    start = (jnp.zeros((D, 3 * D), jnp.float32), jnp.zeros((2 * D,), jnp.float32), jnp.zeros((D, D), jnp.float32), jnp.zeros((D,), jnp.float32), jnp.zeros((D,), jnp.float32), jnp.zeros((D,), jnp.float32), jnp.zeros((D,), jnp.float32), jnp.zeros((D,), jnp.float32), jnp.zeros((D, FF), jnp.float32), jnp.zeros((FF,), jnp.float32), jnp.zeros((FF, D), jnp.float32), jnp.zeros((D,), jnp.float32))
    totals, (output, image_grad) = lax.scan(one_image, start, (images, cotangent))
    return (output, image_grad, totals[0], totals[1], totals[2], totals[3], totals[4], totals[5], totals[6], totals[7], totals[8], totals[9], totals[10], totals[11])
```

```python
import functools

import jax
import jax.numpy as jnp
from jax import lax
from jax.experimental import pallas as pl
from jax.experimental.pallas import tpu as pltpu
from jax.sharding import PartitionSpec as P

HEAD_DIM = 64
LANES = 128
f32 = jnp.float32
bf16 = jnp.bfloat16

epsilon = 1e-06


def norm_stats(matrix):
    mean_val = jnp.mean(matrix, axis=-1, keepdims=True)
    centred = matrix - mean_val
    inv_std = lax.rsqrt(jnp.mean(centred * centred, axis=-1, keepdims=True) + epsilon)
    return (centred * inv_std, inv_std)


def norm_backward(grad_in, normed, inv_std, gain):
    scaled = grad_in * gain
    return inv_std * (
        scaled
        - jnp.mean(scaled, axis=-1, keepdims=True)
        - normed * jnp.mean(scaled * normed, axis=-1, keepdims=True)
    )


def gelu_cdf(pre_act):
    return 0.5 * (1.0 + lax.erf(pre_act * 0.7071067811865476))


def gelu_slope(pre_act):
    return gelu_cdf(pre_act) + pre_act * jnp.exp(-0.5 * pre_act * pre_act) * 0.3989422804014327


def dot(left, right, left_dim=1, right_dim=0):
    return lax.dot_general(
        left, right, (((left_dim,), (right_dim,)), ((), ())), preferred_element_type=f32
    )


def transpose_low(matrix):
    return matrix.astype(f32).T.astype(bf16)


def pair_masks():
    lane = lax.broadcasted_iota(jnp.int32, (1, LANES), 1)
    return (lane < HEAD_DIM, lane >= HEAD_DIM)


def attend_kernel(q_ref, k_ref, v_ref, out_ref, lse_ref, v_flip):
    @pl.when(pl.program_id(1) == 0)
    def _():
        v_flip[...] = transpose_low(v_ref[...])

    query = q_ref[...] * jnp.asarray(HEAD_DIM**-0.5, bf16)
    key = k_ref[...]
    pieces = []
    for head, mask in enumerate(pair_masks()):
        scores = dot(key, jnp.where(mask, query, jnp.zeros_like(query)), 1, 1)
        peak = jnp.max(scores, axis=0, keepdims=True)
        lifted = jnp.exp(scores - peak)
        total = jnp.sum(lifted, axis=0, keepdims=True)
        probs = (lifted * (1.0 / total)).astype(bf16)
        rows = slice(head * HEAD_DIM, (head + 1) * HEAD_DIM)
        pieces.append(dot(v_flip[rows, :], probs))
        lse_ref[0, head : head + 1, :] = peak + jnp.log(total)
    out_ref[...] = jnp.concatenate(pieces, axis=0).T.astype(bf16)


def attend_back_kernel(
    q_ref, k_ref, v_ref, out_ref, grad_ref, lse_ref, all_ref, sums_ref, k_flip, dk_sum, dv_sum
):
    pair, block = pl.program_id(0), pl.program_id(1)
    pairs, blocks = pl.num_programs(0), pl.num_programs(1)
    block_rows = q_ref.shape[0]

    @pl.when(block == 0)
    def _():
        k_flip[...] = transpose_low(k_ref[...])
        dk_sum[...] = jnp.zeros_like(dk_sum)
        dv_sum[...] = jnp.zeros_like(dv_sum)
        sums_ref[...] = jnp.zeros_like(sums_ref)

    query = q_ref[...] * jnp.asarray(HEAD_DIM**-0.5, bf16)
    key = k_ref[...]
    value = v_ref[...]
    grad = grad_ref[...]
    mixed = (grad.astype(f32) * out_ref[...].astype(f32)).T
    pieces = []
    for head, mask in enumerate(pair_masks()):
        rows = slice(head * HEAD_DIM, (head + 1) * HEAD_DIM)
        query_one = jnp.where(mask, query, jnp.zeros_like(query))
        grad_one = jnp.where(mask, grad, jnp.zeros_like(grad))
        probs = jnp.exp(dot(key, query_one, 1, 1) - lse_ref[0, head : head + 1, :])
        prob_grad = dot(value, grad_one, 1, 1)
        delta = jnp.sum(mixed[rows], axis=0, keepdims=True)
        score_grad = (probs * (prob_grad - delta) * HEAD_DIM**-0.5).astype(bf16)
        dv_sum[...] += dot(probs.astype(bf16), grad_one)
        dk_sum[...] += dot(score_grad, query_one)
        pieces.append(dot(k_flip[rows, :], score_grad))
    query_grad = jnp.concatenate(pieces, axis=0).T
    row_at = pl.multiple_of(block * block_rows, block_rows)
    lanes = pl.ds(pl.multiple_of(pair * LANES, LANES), LANES)
    all_ref[pl.ds(row_at, block_rows), lanes] = query_grad.astype(bf16)
    sums_ref[0, 0:1, :] += jnp.sum(query_grad, axis=0, keepdims=True)

    @pl.when(block == blocks - 1)
    def _():
        key_lanes = pl.ds(pl.multiple_of((pairs + pair) * LANES, LANES), LANES)
        value_lanes = pl.ds(pl.multiple_of((2 * pairs + pair) * LANES, LANES), LANES)
        all_ref[:, key_lanes] = (dk_sum[...] * HEAD_DIM**0.5).astype(bf16)
        all_ref[:, value_lanes] = dv_sum[...].astype(bf16)
        sums_ref[0, 1:2, :] = jnp.sum(dv_sum[...], axis=0, keepdims=True)


def block_size(length):
    return next(size for size in (384, 256, 128, length) if length % size == 0)


def attend(projected):
    length, head_cols = projected.shape[0], projected.shape[1] // 3
    pairs = head_cols // LANES
    rows = block_size(length)
    query_spec = pl.BlockSpec((rows, LANES), lambda h, b: (b, h))
    return pl.pallas_call(
        attend_kernel,
        grid=(pairs, length // rows),
        in_specs=[
            query_spec,
            pl.BlockSpec((length, LANES), lambda h, b: (0, pairs + h)),
            pl.BlockSpec((length, LANES), lambda h, b: (0, 2 * pairs + h)),
        ],
        out_specs=[query_spec, pl.BlockSpec((1, 2, rows), lambda h, b: (h, 0, b))],
        out_shape=[
            jax.ShapeDtypeStruct((length, head_cols), bf16),
            jax.ShapeDtypeStruct((pairs, 2, length), f32),
        ],
        scratch_shapes=[pltpu.VMEM((LANES, length), bf16)],
        compiler_params=pltpu.CompilerParams(vmem_limit_bytes=58 * 2**20),
        cost_estimate=pl.CostEstimate(
            flops=16 * pairs * length * length * LANES,
            bytes_accessed=8 * length * head_cols,
            transcendentals=2 * pairs * length * length,
        ),
        name="attend",
    )(projected, projected, projected)


def attend_back(projected, attended, log_total, grad):
    length, head_cols = attended.shape
    pairs = head_cols // LANES
    rows = block_size(length)
    query_spec = pl.BlockSpec((rows, LANES), lambda h, b: (b, h))
    return pl.pallas_call(
        attend_back_kernel,
        grid=(pairs, length // rows),
        in_specs=[
            query_spec,
            pl.BlockSpec((length, LANES), lambda h, b: (0, pairs + h)),
            pl.BlockSpec((length, LANES), lambda h, b: (0, 2 * pairs + h)),
            query_spec,
            query_spec,
            pl.BlockSpec((1, 2, rows), lambda h, b: (h, 0, b)),
        ],
        out_specs=[
            pl.BlockSpec((length, 3 * head_cols), lambda h, b: (0, 0)),
            pl.BlockSpec((1, 2, LANES), lambda h, b: (h, 0, 0)),
        ],
        out_shape=[
            jax.ShapeDtypeStruct((length, 3 * head_cols), bf16),
            jax.ShapeDtypeStruct((pairs, 2, LANES), f32),
        ],
        scratch_shapes=[
            pltpu.VMEM((LANES, length), bf16),
            pltpu.VMEM((length, LANES), f32),
            pltpu.VMEM((length, LANES), f32),
        ],
        compiler_params=pltpu.CompilerParams(vmem_limit_bytes=58 * 2**20),
        cost_estimate=pl.CostEstimate(
            flops=40 * pairs * length * length * LANES,
            bytes_accessed=16 * length * head_cols,
            transcendentals=2 * pairs * length * length,
        ),
        name="attend_back",
    )(projected, projected, projected, attended, grad, log_total)


def body(
    images,
    qkv_weight,
    qv_bias,
    proj_weight,
    proj_bias,
    ln1_gain,
    ln1_bias,
    ln2_gain,
    ln2_bias,
    fc1_weight,
    fc1_bias,
    fc2_weight,
    fc2_bias,
    cotangent,
):
    items, tokens, width = images.shape
    own_rows = items * tokens
    seq_ways, dp_ways = lax.axis_size("seq"), lax.axis_size("dp")
    chips = dp_ways // 2
    shard_rows = width // dp_ways
    column_items = 2 * items
    ranks = seq_ways // column_items
    groups = 2 * ranks
    head_cols = width // groups
    length = seq_ways * tokens
    half = tokens // 2
    dp_index, seq_index = lax.axis_index("dp"), lax.axis_index("seq")
    core, chip = dp_index % 2, dp_index // 2
    first_core = core == 0
    rank = seq_index % ranks
    group = rank * 2 + core
    same_core = [[2 * q + c for q in range(chips)] for c in range(2)]

    def swap(array):
        return lax.ppermute(array, "dp", [(i, i ^ 1) for i in range(dp_ways)])

    def by_core(own, other, axis):
        return jnp.where(
            first_core, jnp.stack([own, other], axis), jnp.stack([other, own], axis)
        )

    def pick(array, index, axis):
        return lax.dynamic_index_in_dim(array, index, axis, keepdims=False)

    def hop(array, bits):
        return lax.ppermute(array, "dp", [(i, i ^ (2 * bits)) for i in range(dp_ways)])

    def gather_chips(block):
        if chips != 4:
            return lax.all_gather(block, "dp", axis=0, axis_index_groups=same_core)
        gathered = jnp.zeros((4,) + block.shape, block.dtype)
        gathered = lax.dynamic_update_index_in_dim(gathered, block, chip, 0)
        for bits in (1, 2, 3):
            gathered = lax.dynamic_update_index_in_dim(gathered, hop(block, bits), chip ^ bits, 0)
        return gathered

    def scatter_chips(blocks):
        if chips != 4:
            return lax.psum_scatter(
                blocks, "dp", scatter_dimension=0, tiled=False, axis_index_groups=same_core
            )
        total = pick(blocks, chip, 0).astype(f32)
        for bits in (1, 2, 3):
            total = total + hop(pick(blocks, chip ^ bits, 0), bits).astype(f32)
        return total.astype(bf16)

    small_names = (qv_bias, proj_bias, ln1_gain, ln1_bias, ln2_gain, ln2_bias, fc1_bias, fc2_bias)
    small = lax.all_gather(jnp.concatenate(small_names), "dp", axis=0)
    smalls, at = [], 0
    for array in small_names:
        smalls.append(small[:, at : at + array.shape[0]].reshape(-1).astype(f32))
        at += array.shape[0]
    qv_full, bias_proj, gain_first, shift_first, gain_second, shift_second, bias_one, bias_two = (
        smalls
    )

    kept = lax.dynamic_slice_in_dim(images, core * half, half, 1)
    given = swap(lax.dynamic_slice_in_dim(images, (1 - core) * half, half, 1))
    column = by_core(kept, given, 0).reshape(column_items, half, width)
    arrived = lax.all_to_all(jnp.repeat(column, ranks, axis=0), "seq", 0, 0)
    image_rows = by_core(arrived, swap(arrived), 1).reshape(length, width).astype(f32)

    qkv_parts = qkv_weight.reshape(shard_rows, 3, groups, head_cols)
    qkv_block = by_core(pick(qkv_parts, group, 2), swap(pick(qkv_parts, group ^ 1, 2)), 0)
    qkv_block = qkv_block.reshape(2 * shard_rows, 3 * head_cols)
    qkv_full = gather_chips(qkv_block).reshape(width, 3 * head_cols)
    proj_full = lax.all_gather(proj_weight, "dp", axis=0, tiled=True)

    fc1_parts = fc1_weight.reshape(shard_rows, chips, 2, -1)
    fc1_block = by_core(pick(fc1_parts, core, 2), swap(pick(fc1_parts, 1 - core, 2)), 0)
    fc1_block = fc1_block.reshape(2 * shard_rows, -1)
    fc1_half = gather_chips(fc1_block).reshape(width, -1)
    fc2_half = gather_chips(fc2_weight).reshape(-1, width)
    bias_one_half = pick(bias_one.reshape(chips, 2, -1), core, 1).reshape(-1)
    cotangent_own = cotangent.reshape(own_rows, width)
    cotangent_all = by_core(cotangent_own, swap(cotangent_own), 0).reshape(2 * own_rows, width)

    bias_parts = qv_full.reshape(2, groups, head_cols)
    bias_group = pick(bias_parts, group, 1)
    bias_row = jnp.concatenate(
        [bias_group[0], jnp.zeros((head_cols,), f32), bias_group[1]]
    )
    normed_image, _ = norm_stats(image_rows)
    hidden_first = (normed_image * gain_first + shift_first).astype(bf16)
    projected = (dot(hidden_first, qkv_full) + bias_row).astype(bf16)
    attended, log_total = attend(projected)

    back = lax.all_to_all(attended.reshape(seq_ways, tokens, head_cols), "seq", 0, 0)
    back = back.reshape(2, items, ranks, tokens, head_cols)
    both = by_core(pick(back, core, 0), swap(pick(back, 1 - core, 0)), 3)
    attended_rows = jnp.moveaxis(both, 1, 2).reshape(own_rows, width)

    flat_rows = images.reshape(own_rows, width).astype(f32)
    residual_first = flat_rows + dot(attended_rows, proj_full) + bias_proj
    normed_second, inv_second = norm_stats(residual_first)
    hidden_own = (normed_second * gain_second + shift_second).astype(bf16)
    hidden_second = by_core(hidden_own, swap(hidden_own), 0).reshape(2 * own_rows, width)
    pre_act = dot(hidden_second, fc1_half) + bias_one_half
    acts = (pre_act * gelu_cdf(pre_act)).astype(bf16)

    def meet(partial):
        parts = partial.reshape(2, own_rows, width)
        return pick(parts, core, 0) + swap(pick(parts, 1 - core, 0).astype(bf16)).astype(f32)

    output = residual_first + meet(dot(acts, fc2_half)) + bias_two

    pre_grad = dot(cotangent_all, fc2_half, 1, 1) * gelu_slope(pre_act)
    pre_grad_low = pre_grad.astype(bf16)
    grad_bias_one = jnp.sum(pre_grad, axis=0)
    grad_out = cotangent_own.astype(f32)
    grad_bias_two = jnp.sum(grad_out, axis=0)
    hidden_second_grad = meet(dot(pre_grad_low, fc1_half, 1, 1))
    grad_gain_second = jnp.sum(hidden_second_grad * normed_second, axis=0)
    grad_shift_second = jnp.sum(hidden_second_grad, axis=0)
    residual_grad = grad_out + norm_backward(
        hidden_second_grad, normed_second, inv_second, gain_second
    )
    residual_grad_low = residual_grad.astype(bf16)
    grad_proj_bias = jnp.sum(residual_grad, axis=0)
    attended_grad = dot(residual_grad_low, proj_full, 1, 1).astype(bf16)
    attended_grad = attended_grad.reshape(items, tokens, ranks, 2, head_cols)
    mine = by_core(
        pick(attended_grad, core, 3), swap(pick(attended_grad, 1 - core, 3)), 0
    ).reshape(column_items, tokens, ranks, head_cols)
    mine = jnp.moveaxis(mine, 2, 1).reshape(seq_ways, tokens, head_cols)
    grad_heads = lax.all_to_all(mine, "seq", 0, 0).reshape(length, head_cols)

    grad_fc_two = dot(acts, cotangent_all, 0, 0).astype(bf16)
    grad_fc_one = dot(hidden_second, pre_grad_low, 0, 0).astype(bf16)
    grad_proj = dot(attended_rows, residual_grad_low, 0, 0).astype(bf16)

    def shares(vector):
        return vector.reshape(dp_ways, -1)

    one_parts = grad_bias_one.reshape(chips, 1, -1)
    one_all = jnp.where(
        jnp.arange(2)[None, :, None] == core, jnp.broadcast_to(one_parts, (chips, 2, one_parts.shape[2])), 0.0
    )
    extra = jnp.concatenate(
        [
            shares(grad_proj_bias),
            shares(grad_gain_second),
            shares(grad_shift_second),
            shares(grad_bias_two),
            shares(one_all),
        ],
        axis=1,
    ).astype(bf16)
    extra = jnp.pad(extra[:, None, :], ((0, 0), (0, 15), (0, width - extra.shape[1])))
    proj_blocks = jnp.concatenate([grad_proj.reshape(dp_ways, shard_rows, width), extra], axis=1)

    share_two = scatter_chips(grad_fc_two.reshape(chips, -1, width))
    share_one = scatter_chips(grad_fc_one.reshape(chips, 2 * shard_rows, -1))
    share_proj = lax.psum_scatter(proj_blocks, "dp", scatter_dimension=0, tiled=True)[0]
    share_two = lax.psum(share_two, "seq")
    share_one, share_two = lax.optimization_barrier((share_one, share_two))
    share_one = lax.psum(share_one, "seq")
    share_proj, share_one = lax.optimization_barrier((share_proj, share_one))
    share_proj = lax.psum(share_proj, "seq")

    qkv_grad, bias_sums = attend_back(projected, attended, log_total, grad_heads)
    hidden_partial = dot(qkv_grad, qkv_full, 1, 1)
    grad_gain_first = jnp.sum(hidden_partial * normed_image, axis=0)
    grad_shift_first = jnp.sum(hidden_partial, axis=0)
    partial_parts = hidden_partial.reshape(seq_ways, 2, half, width)
    chip_sum = pick(partial_parts, core, 1) + swap(
        pick(partial_parts, 1 - core, 1).astype(bf16)
    ).astype(f32)
    home = lax.all_to_all(chip_sum.astype(bf16), "seq", 0, 0)
    home = home.reshape(2, items, ranks, half, width)
    if ranks > 1:
        home = jnp.sum(home.astype(f32), axis=2, keepdims=True).astype(bf16)
    home = home[:, :, 0]
    hidden_first_grad = by_core(pick(home, core, 0), swap(pick(home, 1 - core, 0)), 1)
    hidden_first_grad = hidden_first_grad.reshape(own_rows, width).astype(f32)
    normed_first, inv_first = norm_stats(flat_rows)
    image_grad = residual_grad + norm_backward(
        hidden_first_grad, normed_first, inv_first, gain_first
    )

    grad_qkv = dot(hidden_first, qkv_grad, 0, 0).astype(bf16)
    grad_qkv = grad_qkv.reshape(chips, 2 * shard_rows, 3, 1, head_cols)
    qv_sums = jnp.moveaxis(bias_sums, 1, 0).reshape(2, 1, head_cols)
    qv_all = lax.dynamic_update_slice(jnp.zeros((2, groups, head_cols), f32), qv_sums, (0, group, 0))
    extra = jnp.concatenate(
        [
            grad_gain_first.reshape(chips, -1),
            grad_shift_first.reshape(chips, -1),
            qv_all.reshape(chips, -1),
        ],
        axis=1,
    ).astype(bf16)
    extra_cols = extra.shape[1]
    extra = jnp.pad(extra[:, None, :], ((0, 0), (0, 15), (0, 3 * head_cols - extra_cols)))
    blocks = jnp.concatenate(
        [grad_qkv.reshape(chips, 2 * shard_rows, 3 * head_cols), extra], axis=1
    )
    share_qkv = scatter_chips(blocks)
    extra = share_qkv[2 * shard_rows, :extra_cols]
    share_qkv = share_qkv[: 2 * shard_rows].reshape(2 * shard_rows, 3, 1, head_cols)
    if ranks > 1:
        share_qkv = lax.dynamic_update_slice(
            jnp.zeros((2 * shard_rows, 3, ranks, head_cols), bf16), share_qkv, (0, 0, rank, 0)
        )
    flat = jnp.concatenate(
        [
            share_qkv.reshape(2 * shard_rows, -1),
            jnp.pad(extra[None], ((0, 15), (0, ranks * 3 * head_cols - extra_cols))),
        ],
        axis=0,
    )
    flat, share_proj = lax.optimization_barrier((flat, share_proj))
    flat = lax.psum(flat, "seq")
    rows_parts = flat[: 2 * shard_rows].reshape(2, shard_rows, 3, ranks, head_cols)
    extra = flat[2 * shard_rows : 2 * shard_rows + 1]
    out_qkv = by_core(pick(rows_parts, core, 0), swap(pick(rows_parts, 1 - core, 0)), 3)
    out_qkv = out_qkv.reshape(shard_rows, 3 * width).astype(f32)
    extra = (extra.astype(f32) + swap(extra).astype(f32))[0]
    per_chip = width // chips
    out_gain_first = pick(extra[:per_chip].reshape(2, -1), core, 0)
    out_shift_first = pick(extra[per_chip : 2 * per_chip].reshape(2, -1), core, 0)
    out_qv = pick(extra[2 * per_chip : 4 * per_chip].reshape(2, -1), core, 0)

    one_rows = share_one.reshape(2, shard_rows, chips, -1)
    out_one = by_core(pick(one_rows, core, 0), swap(pick(one_rows, 1 - core, 0)), 2)
    out_one = out_one.reshape(shard_rows, -1).astype(f32)
    last = share_proj[shard_rows].astype(f32)
    out_smalls, at = [], 0
    for size in (shard_rows, shard_rows, shard_rows, shard_rows, 4 * shard_rows):
        out_smalls.append(last[at : at + size])
        at += size
    return (
        output.reshape(images.shape),
        image_grad.reshape(images.shape),
        out_qkv,
        out_qv,
        share_proj[:shard_rows].astype(f32),
        out_smalls[0],
        out_gain_first,
        out_shift_first,
        out_smalls[1],
        out_smalls[2],
        out_one,
        out_smalls[4],
        share_two.astype(f32),
        out_smalls[3],
    )


def solution(mesh):
    rows, cols, flat = P("dp", "seq", None), P("dp", None), P("dp")
    in_specs = (rows, cols, flat, cols, flat, flat, flat, flat, flat, cols, flat, cols, flat, rows)
    out_specs = (rows, rows, cols, flat, cols, flat, flat, flat, flat, flat, cols, flat, cols, flat)
    return jax.shard_map(body, mesh=mesh, in_specs=in_specs, out_specs=out_specs, check_vma=False)
```

```python
import functools

import jax
import jax.numpy as jnp
from jax import lax
from jax.experimental import pallas as pl
from jax.experimental.pallas import tpu as pltpu
from jax.sharding import PartitionSpec as P

HEAD_DIM = 64
LANES = 128
f32 = jnp.float32
bf16 = jnp.bfloat16

epsilon = 1e-06


def norm_stats(matrix):
    mean_val = jnp.mean(matrix, axis=-1, keepdims=True)
    centred = matrix - mean_val
    inv_std = lax.rsqrt(jnp.mean(centred * centred, axis=-1, keepdims=True) + epsilon)
    return (centred * inv_std, inv_std)


def norm_backward(grad_in, normed, inv_std, gain):
    scaled = grad_in * gain
    return inv_std * (
        scaled
        - jnp.mean(scaled, axis=-1, keepdims=True)
        - normed * jnp.mean(scaled * normed, axis=-1, keepdims=True)
    )


def gelu_cdf(pre_act):
    return 0.5 * (1.0 + lax.erf(pre_act * 0.7071067811865476))


def gelu_slope(pre_act):
    return gelu_cdf(pre_act) + pre_act * jnp.exp(-0.5 * pre_act * pre_act) * 0.3989422804014327


def dot(left, right, left_dim=1, right_dim=0):
    return lax.dot_general(
        left, right, (((left_dim,), (right_dim,)), ((), ())), preferred_element_type=f32
    )


def transpose_low(matrix):
    return matrix.astype(f32).T.astype(bf16)


def pair_masks():
    lane = lax.broadcasted_iota(jnp.int32, (1, LANES), 1)
    return (lane < HEAD_DIM, lane >= HEAD_DIM)


def attend_kernel(q_ref, k_ref, v_ref, out_ref, lse_ref, v_flip):
    @pl.when(pl.program_id(1) == 0)
    def _():
        v_flip[...] = transpose_low(v_ref[...])

    query = q_ref[...] * jnp.asarray(HEAD_DIM**-0.5, bf16)
    key = k_ref[...]
    pieces = []
    for head, mask in enumerate(pair_masks()):
        scores = dot(key, jnp.where(mask, query, jnp.zeros_like(query)), 1, 1)
        peak = jnp.max(scores, axis=0, keepdims=True)
        lifted = jnp.exp(scores - peak)
        total = jnp.sum(lifted, axis=0, keepdims=True)
        probs = (lifted * (1.0 / total)).astype(bf16)
        rows = slice(head * HEAD_DIM, (head + 1) * HEAD_DIM)
        pieces.append(dot(v_flip[rows, :], probs))
        lse_ref[0, head : head + 1, :] = peak + jnp.log(total)
    out_ref[...] = jnp.concatenate(pieces, axis=0).T.astype(bf16)


def attend_back_kernel(
    q_ref, k_ref, v_ref, out_ref, grad_ref, lse_ref, all_ref, sums_ref, k_flip, dk_sum, dv_sum
):
    pair, block = pl.program_id(0), pl.program_id(1)
    pairs, blocks = pl.num_programs(0), pl.num_programs(1)
    block_rows = q_ref.shape[0]

    @pl.when(block == 0)
    def _():
        k_flip[...] = transpose_low(k_ref[...])
        dk_sum[...] = jnp.zeros_like(dk_sum)
        dv_sum[...] = jnp.zeros_like(dv_sum)
        sums_ref[...] = jnp.zeros_like(sums_ref)

    query = q_ref[...] * jnp.asarray(HEAD_DIM**-0.5, bf16)
    key = k_ref[...]
    value = v_ref[...]
    grad = grad_ref[...]
    mixed = (grad.astype(f32) * out_ref[...].astype(f32)).T
    pieces = []
    for head, mask in enumerate(pair_masks()):
        rows = slice(head * HEAD_DIM, (head + 1) * HEAD_DIM)
        query_one = jnp.where(mask, query, jnp.zeros_like(query))
        grad_one = jnp.where(mask, grad, jnp.zeros_like(grad))
        probs = jnp.exp(dot(key, query_one, 1, 1) - lse_ref[0, head : head + 1, :])
        prob_grad = dot(value, grad_one, 1, 1)
        delta = jnp.sum(mixed[rows], axis=0, keepdims=True)
        score_grad = (probs * (prob_grad - delta) * HEAD_DIM**-0.5).astype(bf16)
        dv_sum[...] += dot(probs.astype(bf16), grad_one)
        dk_sum[...] += dot(score_grad, query_one)
        pieces.append(dot(k_flip[rows, :], score_grad))
    query_grad = jnp.concatenate(pieces, axis=0).T
    row_at = pl.multiple_of(block * block_rows, block_rows)
    lanes = pl.ds(pl.multiple_of(pair * LANES, LANES), LANES)
    all_ref[pl.ds(row_at, block_rows), lanes] = query_grad.astype(bf16)
    sums_ref[0, 0:1, :] += jnp.sum(query_grad, axis=0, keepdims=True)

    @pl.when(block == blocks - 1)
    def _():
        key_lanes = pl.ds(pl.multiple_of((pairs + pair) * LANES, LANES), LANES)
        value_lanes = pl.ds(pl.multiple_of((2 * pairs + pair) * LANES, LANES), LANES)
        all_ref[:, key_lanes] = (dk_sum[...] * HEAD_DIM**0.5).astype(bf16)
        all_ref[:, value_lanes] = dv_sum[...].astype(bf16)
        sums_ref[0, 1:2, :] = jnp.sum(dv_sum[...], axis=0, keepdims=True)


def block_size(length):
    return next(size for size in (384, 256, 128, length) if length % size == 0)


def attend(projected):
    length, head_cols = projected.shape[0], projected.shape[1] // 3
    pairs = head_cols // LANES
    rows = block_size(length)
    query_spec = pl.BlockSpec((rows, LANES), lambda h, b: (b, h))
    return pl.pallas_call(
        attend_kernel,
        grid=(pairs, length // rows),
        in_specs=[
            query_spec,
            pl.BlockSpec((length, LANES), lambda h, b: (0, pairs + h)),
            pl.BlockSpec((length, LANES), lambda h, b: (0, 2 * pairs + h)),
        ],
        out_specs=[query_spec, pl.BlockSpec((1, 2, rows), lambda h, b: (h, 0, b))],
        out_shape=[
            jax.ShapeDtypeStruct((length, head_cols), bf16),
            jax.ShapeDtypeStruct((pairs, 2, length), f32),
        ],
        scratch_shapes=[pltpu.VMEM((LANES, length), bf16)],
        compiler_params=pltpu.CompilerParams(vmem_limit_bytes=58 * 2**20),
        cost_estimate=pl.CostEstimate(
            flops=16 * pairs * length * length * LANES,
            bytes_accessed=8 * length * head_cols,
            transcendentals=2 * pairs * length * length,
        ),
        name="attend",
    )(projected, projected, projected)


def attend_back(projected, attended, log_total, grad):
    length, head_cols = attended.shape
    pairs = head_cols // LANES
    rows = block_size(length)
    query_spec = pl.BlockSpec((rows, LANES), lambda h, b: (b, h))
    return pl.pallas_call(
        attend_back_kernel,
        grid=(pairs, length // rows),
        in_specs=[
            query_spec,
            pl.BlockSpec((length, LANES), lambda h, b: (0, pairs + h)),
            pl.BlockSpec((length, LANES), lambda h, b: (0, 2 * pairs + h)),
            query_spec,
            query_spec,
            pl.BlockSpec((1, 2, rows), lambda h, b: (h, 0, b)),
        ],
        out_specs=[
            pl.BlockSpec((length, 3 * head_cols), lambda h, b: (0, 0)),
            pl.BlockSpec((1, 2, LANES), lambda h, b: (h, 0, 0)),
        ],
        out_shape=[
            jax.ShapeDtypeStruct((length, 3 * head_cols), bf16),
            jax.ShapeDtypeStruct((pairs, 2, LANES), f32),
        ],
        scratch_shapes=[
            pltpu.VMEM((LANES, length), bf16),
            pltpu.VMEM((length, LANES), f32),
            pltpu.VMEM((length, LANES), f32),
        ],
        compiler_params=pltpu.CompilerParams(vmem_limit_bytes=58 * 2**20),
        cost_estimate=pl.CostEstimate(
            flops=40 * pairs * length * length * LANES,
            bytes_accessed=16 * length * head_cols,
            transcendentals=2 * pairs * length * length,
        ),
        name="attend_back",
    )(projected, projected, projected, attended, grad, log_total)


class Copies:
    def __init__(self, send_sems, recv_sems, local_sems):
        self.send_sems, self.recv_sems, self.local_sems = send_sems, recv_sems, local_sems
        self.sent, self.locals, self.local_count = [], [], 0

    def remote(self, src, dst, **device):
        at = len(self.sent)
        copy = pltpu.make_async_remote_copy(
            src_ref=src,
            dst_ref=dst,
            send_sem=self.send_sems.at[at],
            recv_sem=self.recv_sems.at[at],
            device_id=device,
            device_id_type=pl.DeviceIdType.MESH,
        )
        copy.start()
        self.sent.append(copy)
        return copy

    def local(self, src, dst):
        copy = pltpu.make_async_copy(src, dst, self.local_sems.at[self.local_count])
        copy.start()
        self.locals.append(copy)
        self.local_count += 1
        return copy

    def wait_local(self, copy):
        copy.wait()
        self.locals = [kept for kept in self.locals if kept is not copy]

    def finish(self):
        for copy in self.sent:
            copy.wait_send()
        for copy in self.locals:
            copy.wait()


class Place:
    def __init__(self, items):
        self.dp_ways, self.seq_ways = lax.axis_size("dp"), lax.axis_size("seq")
        self.chips = self.dp_ways // 2
        self.ranks = self.seq_ways // (2 * items)
        self.dp, self.seq = lax.axis_index("dp"), lax.axis_index("seq")
        self.core, self.chip = lax.rem(self.dp, 2), lax.div(self.dp, 2)
        self.rank = lax.rem(self.seq, self.ranks)
        self.item = lax.div(self.seq, self.ranks)

    def partner(self, offset):
        if self.chips == 4:
            x, y = lax.rem(self.chip, 2), lax.div(self.chip, 2)
            x = 1 - x if offset % 2 else x
            y = 1 - y if offset >= 2 else y
            return y * 2 + x
        return lax.rem(self.chip + offset, self.chips)

    def source(self, offset):
        if self.chips == 4:
            return self.partner(offset)
        return lax.rem(self.chip + self.chips - offset, self.chips)

    def meet(self):
        barrier = pltpu.get_barrier_semaphore()
        for step in range(1, self.dp_ways):
            pl.semaphore_signal(
                barrier,
                inc=1,
                device_id={"dp": lax.rem(self.dp + step, self.dp_ways)},
                device_id_type=pl.DeviceIdType.MESH,
            )
        for step in range(1, self.seq_ways):
            for core in range(2):
                pl.semaphore_signal(
                    barrier,
                    inc=1,
                    device_id={
                        "dp": self.chip * 2 + core,
                        "seq": lax.rem(self.seq + step, self.seq_ways),
                    },
                    device_id_type=pl.DeviceIdType.MESH,
                )
        pl.semaphore_wait(barrier, self.dp_ways - 1 + 2 * (self.seq_ways - 1))


def rows_at(start, size):
    return pl.ds(pl.multiple_of(start, 16), size)


def lanes_at(start, size):
    return pl.ds(pl.multiple_of(start, LANES), size)


def attend_rows(prj, out, lse, v_flip, pair, block, rows):
    pairs = out.shape[1] // LANES
    query = prj[rows_at(block * rows, rows), lanes_at(pair * LANES, LANES)]
    query = query * jnp.asarray(HEAD_DIM**-0.5, bf16)
    key = prj[:, lanes_at((pairs + pair) * LANES, LANES)]
    pieces = []
    for head, mask in enumerate(pair_masks()):
        scores = dot(key, jnp.where(mask, query, jnp.zeros_like(query)), 1, 1)
        peak = jnp.max(scores, axis=0, keepdims=True)
        lifted = jnp.exp(scores - peak)
        total = jnp.sum(lifted, axis=0, keepdims=True)
        probs = (lifted * (1.0 / total)).astype(bf16)
        pieces.append(dot(v_flip[head * HEAD_DIM : (head + 1) * HEAD_DIM, :], probs))
        lse[pair, head : head + 1, lanes_at(block * rows, rows)] = peak + jnp.log(total)
    out[rows_at(block * rows, rows), lanes_at(pair * LANES, LANES)] = (
        jnp.concatenate(pieces, axis=0).T.astype(bf16)
    )


def forward_kernel(
    items,
    img,
    wq,
    wp,
    w1,
    w2,
    cot,
    small,
    img_out,
    wq_out,
    wp_out,
    w1_out,
    w2_out,
    cot_out,
    small_out,
    prj_out,
    heads_out,
    lse_out,
    rows_out,
    img_v,
    wq_v,
    prj_v,
    heads_v,
    small_v,
    vec_v,
    v_flip,
    send_sems,
    recv_sems,
    local_sems,
    swap_sems,
    token_send,
    token_recv,
    back_send,
    back_recv,
):
    at = Place(items)
    chips, ranks, seq_ways, dp_ways = at.chips, at.ranks, at.seq_ways, at.dp_ways
    tokens = img.shape[0] // items
    half = tokens // 2
    shard, width = wp.shape
    head_cols = heads_v.shape[1]
    unit_rows = w2.shape[0]
    length = img_v.shape[0]
    pairs = head_cols // LANES
    relay = chips == 4
    offsets = (1, 2) if relay else tuple(range(1, chips))
    copies = Copies(send_sems, recv_sems, local_sems)
    at.meet()
    me = rows_at(at.dp * shard, shard)

    token_jobs = []
    for item in range(items):
        for k in range(ranks):
            for h in range(2):
                to_seq = (at.core * items + item) * ranks + k
                mine = (to_seq == at.seq) & (at.core == h)
                src = img.at[pl.ds(item * tokens + h * half, half), :]
                dst = img_v.at[rows_at(at.seq * tokens + h * half, half), :]
                sem = token_send.at[len(token_jobs)]
                far = pltpu.make_async_remote_copy(
                    src_ref=src,
                    dst_ref=dst,
                    send_sem=sem,
                    recv_sem=token_recv.at[at.seq],
                    device_id={"dp": at.chip * 2 + h, "seq": to_seq},
                    device_id_type=pl.DeviceIdType.MESH,
                )
                near = pltpu.make_async_copy(src, dst, token_recv.at[at.seq])
                pl.when(mine)(near.start)
                pl.when(jnp.logical_not(mine))(far.start)
                token_jobs.append((mine, far))

    other = at.chip * 2 + 1 - at.core
    small_copies = []
    small_rows = pl.ds(pl.multiple_of(at.dp * 8, 8), 8)
    small_own = copies.local(small, small_v.at[small_rows, :])
    for step in range(1, dp_ways):
        small_copies.append(
            copies.remote(small, small_v.at[small_rows, :], dp=lax.rem(at.dp + step, dp_ways))
        )

    def qkv_pieces(core):
        group = at.rank * 2 + core
        return [
            (
                wq.at[:, lanes_at(part * width + group * head_cols, head_cols)],
                wq_v.at[me, pl.ds(part * head_cols, head_cols)],
            )
            for part in range(3)
        ]

    def fc1_pieces(core):
        return [
            (
                w1.at[:, lanes_at((2 * q + core) * unit_rows, unit_rows)],
                w1_out.at[me, pl.ds(q * unit_rows, unit_rows)],
            )
            for q in range(chips)
        ]

    def start_columns(pieces):
        arrivals = {0: [], "local": [copies.local(src, dst) for src, dst in pieces(at.core)]}
        for src, dst in pieces(1 - at.core):
            arrivals[0].append(copies.remote(src, dst, dp=other))
        for offset in offsets:
            for core in (at.core, 1 - at.core):
                for src, dst in pieces(core):
                    copy = copies.remote(src, dst, dp=at.partner(offset) * 2 + core)
                    arrivals.setdefault(offset, []).append(copy)
        return arrivals

    def pass_on(arrivals, block_of, first, second):
        for copy in arrivals[1]:
            copy.wait_recv()
        last = []
        if relay:
            ref = block_of(at.partner(1), *first)
            last.append(copies.remote(ref, ref, dp=at.partner(2) * 2 + at.core))
        for copy in arrivals[2]:
            copy.wait_recv()
        if relay:
            ref = block_of(at.partner(2), *second)
            last.append(copies.remote(ref, ref, dp=at.partner(1) * 2 + at.core))
        for offset in range(3, chips):
            if not relay:
                for copy in arrivals[offset]:
                    copy.wait_recv()
        return last

    def settle(arrivals, last):
        for copy in last:
            copy.wait_recv()
        for copy in arrivals[0]:
            copy.wait_recv()

    def shard_halves(ref):
        return lambda chip, start, size: ref.at[rows_at(chip * 2 * shard + start, size), :]

    qkv_arrivals = start_columns(qkv_pieces)

    wp_near = [copies.remote(wp, wp_out.at[me, :], dp=other)]
    copies.local(wp, wp_out.at[me, :])
    wp_far = {
        o: [copies.remote(wp, wp_out.at[me, :], dp=at.partner(o) * 2 + at.core)] for o in offsets
    }
    cot_rows = rows_at(at.core * cot.shape[0], cot.shape[0])
    cot_near = copies.remote(cot, cot_out.at[cot_rows, :], dp=other)
    copies.local(cot, cot_out.at[cot_rows, :])

    for s in range(seq_ways):
        pltpu.make_async_copy(
            img.at[pl.ds(0, half), :], img_v.at[pl.ds(s * tokens, half), :], token_recv.at[s]
        ).wait()
    for mine, far in token_jobs:
        pl.when(jnp.logical_not(mine))(far.wait_send)
    token_near = []
    for s in range(seq_ways):
        ref = img_v.at[rows_at(s * tokens + at.core * half, half), :]
        token_near.append(copies.remote(ref, ref, dp=other))
    qkv_last = pass_on(qkv_arrivals, shard_halves(wq_v), (0, shard), (shard, shard))
    fc1_arrivals = start_columns(fc1_pieces)
    w2_to = lambda chip: w2_out.at[rows_at(chip * unit_rows, unit_rows), :]
    copies.local(w2, w2_to(at.chip))
    fc2_arrivals = {0: []}
    for offset in offsets:
        fc2_arrivals[offset] = [
            copies.remote(w2, w2_to(at.chip), dp=at.partner(offset) * 2 + at.core)
        ]

    for copy in small_copies:
        copy.wait_recv()
    copies.wait_local(small_own)
    names = {"query": (0, 2), "gain": (3, 1), "shift": (4, 1)}
    for row, (start, size) in enumerate(names.values()):
        for i in range(dp_ways):
            vec_v[row : row + 1, i * size * shard : (i + 1) * size * shard] = small_v[
                8 * i : 8 * i + 1, start * shard : (start + size) * shard
            ]
    for copy in token_near:
        copy.wait_recv()
    settle(qkv_arrivals, qkv_last)
    for copy in qkv_arrivals["local"]:
        copies.wait_local(copy)

    group = at.rank * 2 + at.core
    gain = vec_v[1:2, :width]
    shift = vec_v[2:3, :width]

    def project(step, carry):
        rows = rows_at(step * tokens, tokens)
        normed, _ = norm_stats(img_v[rows, :].astype(f32))
        hidden = (normed * gain + shift).astype(bf16)
        for part in range(3):
            cols = slice(part * head_cols, (part + 1) * head_cols)
            block = dot(hidden, wq_v[:, cols])
            if part != 1:
                lanes = lanes_at((part // 2) * width + group * head_cols, head_cols)
                block = block + vec_v[0:1, lanes]
            prj_v[rows, cols] = block.astype(bf16)
        return carry

    lax.fori_loop(0, seq_ways, project, 0)
    copies.local(img_v, img_out)
    copies.local(wq_v, wq_out)
    copies.local(prj_v, prj_out)
    copies.local(small_v, small_out)

    rows = block_size(length)
    home_core = lax.div(at.item, items)
    home_item = lax.rem(at.item, items)

    def back_copies(pair):
        jobs = []
        for s in range(seq_ways):
            mine = (at.seq == s) & (at.core == home_core)
            src = heads_v.at[pl.ds(s * tokens, tokens), lanes_at(pair * LANES, LANES)]
            dst = rows_out.at[
                rows_at(home_item * tokens, tokens),
                lanes_at(group * head_cols + pair * LANES, LANES),
            ]
            far = pltpu.make_async_remote_copy(
                src_ref=src,
                dst_ref=dst,
                send_sem=back_send.at[pair, s],
                recv_sem=back_recv,
                device_id={"dp": at.chip * 2 + home_core, "seq": s},
                device_id_type=pl.DeviceIdType.MESH,
            )
            near = pltpu.make_async_copy(src, dst, back_recv)
            jobs.append((mine, far, near))
        return jobs

    def one_pair(pair, carry):
        v_flip[...] = transpose_low(prj_v[:, lanes_at((2 * pairs + pair) * LANES, LANES)])

        def one_block(block, inner):
            attend_rows(prj_v, heads_v, lse_out, v_flip, pair, block, rows)
            return inner

        lax.fori_loop(0, length // rows, one_block, 0)
        for mine, far, near in back_copies(pair):
            pl.when(mine)(near.start)
            pl.when(jnp.logical_not(mine))(far.start)
        return carry

    lax.fori_loop(0, pairs, one_pair, 0)
    copies.local(heads_v, heads_out)
    wp_last = pass_on(
        wp_far,
        lambda chip, start, size: wp_out.at[
            rows_at((chip * 2 + at.core) * shard + start, size), :
        ],
        (0, shard // 2),
        (shard // 2, shard // 2),
    )
    fc1_last = pass_on(fc1_arrivals, shard_halves(w1_out), (0, shard), (shard, shard))
    for copy in wp_last:
        copy.wait_recv()
    for offset in range(1, chips):
        ref = wp_out.at[rows_at((at.source(offset) * 2 + at.core) * shard, shard), :]
        wp_near.append(copies.remote(ref, ref, dp=other))
    fc2_last = pass_on(
        fc2_arrivals,
        lambda chip, start, size: w2_out.at[rows_at(chip * unit_rows + start, size), :],
        (0, unit_rows // 2),
        (unit_rows // 2, unit_rows // 2),
    )
    settle(fc1_arrivals, fc1_last)
    settle(fc2_arrivals, fc2_last)
    for copy in wp_near:
        copy.wait_recv()
    cot_near.wait_recv()
    pltpu.make_async_copy(rows_out, rows_out, back_recv).wait()

    def drain(pair, carry):
        for mine, far, _ in back_copies(pair):
            pl.when(jnp.logical_not(mine))(far.wait_send)
        return carry

    lax.fori_loop(0, pairs, drain, 0)
    copies.finish()


def forward(items, img, wq, wp, w1, w2, cot, small):
    dp_ways, seq_ways = lax.axis_size("dp"), lax.axis_size("seq")
    ranks = seq_ways // (2 * items)
    shard, width = wp.shape
    head_cols = width // (2 * ranks)
    tokens = img.shape[0] // items
    length = seq_ways * tokens
    half_units = w1.shape[1] // 2
    pairs = head_cols // LANES
    any_spec = pl.BlockSpec(memory_space=pl.ANY)
    out_shape = [
        jax.ShapeDtypeStruct((length, width), bf16),
        jax.ShapeDtypeStruct((width, 3 * head_cols), bf16),
        jax.ShapeDtypeStruct((width, width), bf16),
        jax.ShapeDtypeStruct((width, half_units), bf16),
        jax.ShapeDtypeStruct((half_units, width), bf16),
        jax.ShapeDtypeStruct((2 * cot.shape[0], width), bf16),
        jax.ShapeDtypeStruct((8 * dp_ways, small.shape[1]), f32),
        jax.ShapeDtypeStruct((length, 3 * head_cols), bf16),
        jax.ShapeDtypeStruct((length, head_cols), bf16),
        jax.ShapeDtypeStruct((pairs, 2, length), f32),
        jax.ShapeDtypeStruct(img.shape, bf16),
    ]
    out_specs = [any_spec] * len(out_shape)
    out_specs[9] = pl.BlockSpec(memory_space=pltpu.VMEM)
    remotes = 160
    return pl.pallas_call(
        functools.partial(forward_kernel, items),
        in_specs=[any_spec] * 7,
        out_specs=out_specs,
        out_shape=out_shape,
        scratch_shapes=[
            pltpu.VMEM((length, width), bf16),
            pltpu.VMEM((width, 3 * head_cols), bf16),
            pltpu.VMEM((length, 3 * head_cols), bf16),
            pltpu.VMEM((length, head_cols), bf16),
            pltpu.VMEM((8 * dp_ways, small.shape[1]), f32),
            pltpu.VMEM((8, 2 * width), f32),
            pltpu.VMEM((LANES, length), bf16),
            pltpu.SemaphoreType.DMA((remotes,)),
            pltpu.SemaphoreType.DMA((remotes,)),
            pltpu.SemaphoreType.DMA((32,)),
            pltpu.SemaphoreType.DMA((2,)),
            pltpu.SemaphoreType.DMA((2 * items * ranks,)),
            pltpu.SemaphoreType.DMA((seq_ways,)),
            pltpu.SemaphoreType.DMA((pairs, seq_ways)),
            pltpu.SemaphoreType.DMA,
        ],
        compiler_params=pltpu.CompilerParams(
            collective_id=0, has_side_effects=True, vmem_limit_bytes=62 * 2**20
        ),
        name="forward",
    )(img, wq, wp, w1, w2, cot, small)


def body(
    images,
    qkv_weight,
    qv_bias,
    proj_weight,
    proj_bias,
    ln1_gain,
    ln1_bias,
    ln2_gain,
    ln2_bias,
    fc1_weight,
    fc1_bias,
    fc2_weight,
    fc2_bias,
    cotangent,
):
    items, tokens, width = images.shape
    own_rows = items * tokens
    seq_ways, dp_ways = lax.axis_size("seq"), lax.axis_size("dp")
    chips = dp_ways // 2
    shard_rows = width // dp_ways
    column_items = 2 * items
    ranks = seq_ways // column_items
    groups = 2 * ranks
    head_cols = width // groups
    length = seq_ways * tokens
    half = tokens // 2
    dp_index, seq_index = lax.axis_index("dp"), lax.axis_index("seq")
    core, chip = dp_index % 2, dp_index // 2
    first_core = core == 0
    rank = seq_index % ranks
    group = rank * 2 + core
    same_core = [[2 * q + c for q in range(chips)] for c in range(2)]

    def swap(array):
        return lax.ppermute(array, "dp", [(i, i ^ 1) for i in range(dp_ways)])

    def by_core(own, other, axis):
        return jnp.where(
            first_core, jnp.stack([own, other], axis), jnp.stack([other, own], axis)
        )

    def pick(array, index, axis):
        return lax.dynamic_index_in_dim(array, index, axis, keepdims=False)

    def hop(array, bits):
        return lax.ppermute(array, "dp", [(i, i ^ (2 * bits)) for i in range(dp_ways)])

    def gather_chips(block):
        if chips != 4:
            return lax.all_gather(block, "dp", axis=0, axis_index_groups=same_core)
        gathered = jnp.zeros((4,) + block.shape, block.dtype)
        gathered = lax.dynamic_update_index_in_dim(gathered, block, chip, 0)
        for bits in (1, 2, 3):
            gathered = lax.dynamic_update_index_in_dim(gathered, hop(block, bits), chip ^ bits, 0)
        return gathered

    def scatter_chips(blocks):
        if chips != 4:
            return lax.psum_scatter(
                blocks, "dp", scatter_dimension=0, tiled=False, axis_index_groups=same_core
            )
        total = pick(blocks, chip, 0).astype(f32)
        for bits in (1, 2, 3):
            total = total + hop(pick(blocks, chip ^ bits, 0), bits).astype(f32)
        return total.astype(bf16)

    small_names = (qv_bias, proj_bias, ln1_gain, ln1_bias, ln2_gain, ln2_bias, fc1_bias, fc2_bias)
    small = jnp.concatenate(small_names).astype(f32)
    cotangent_own = cotangent.reshape(own_rows, width)
    (
        image_low,
        qkv_full,
        proj_full,
        fc1_half,
        fc2_half,
        cotangent_all,
        small,
        projected,
        attended,
        log_total,
        attended_rows,
    ) = forward(
        items,
        images.reshape(own_rows, width),
        qkv_weight,
        proj_weight,
        fc1_weight,
        fc2_weight,
        cotangent_own,
        jnp.broadcast_to(small, (8, small.shape[0])),
    )
    small = small.reshape(dp_ways, 8, -1)[:, 0]
    smalls, at = [], 0
    for array in small_names:
        smalls.append(small[:, at : at + array.shape[0]].reshape(-1))
        at += array.shape[0]
    _, bias_proj, gain_first, shift_first, gain_second, shift_second, bias_one, bias_two = smalls
    bias_one_half = pick(bias_one.reshape(chips, 2, -1), core, 1).reshape(-1)
    normed_image, _ = norm_stats(image_low.astype(f32))
    hidden_first = (normed_image * gain_first + shift_first).astype(bf16)

    flat_rows = images.reshape(own_rows, width).astype(f32)
    residual_first = flat_rows + dot(attended_rows, proj_full) + bias_proj
    normed_second, inv_second = norm_stats(residual_first)
    hidden_own = (normed_second * gain_second + shift_second).astype(bf16)
    hidden_second = by_core(hidden_own, swap(hidden_own), 0).reshape(2 * own_rows, width)
    pre_act = dot(hidden_second, fc1_half) + bias_one_half
    acts = (pre_act * gelu_cdf(pre_act)).astype(bf16)

    def meet(partial):
        parts = partial.reshape(2, own_rows, width)
        return pick(parts, core, 0) + swap(pick(parts, 1 - core, 0).astype(bf16)).astype(f32)

    output = residual_first + meet(dot(acts, fc2_half)) + bias_two

    pre_grad = dot(cotangent_all, fc2_half, 1, 1) * gelu_slope(pre_act)
    pre_grad_low = pre_grad.astype(bf16)
    grad_bias_one = jnp.sum(pre_grad, axis=0)
    grad_out = cotangent_own.astype(f32)
    grad_bias_two = jnp.sum(grad_out, axis=0)
    hidden_second_grad = meet(dot(pre_grad_low, fc1_half, 1, 1))
    grad_gain_second = jnp.sum(hidden_second_grad * normed_second, axis=0)
    grad_shift_second = jnp.sum(hidden_second_grad, axis=0)
    residual_grad = grad_out + norm_backward(
        hidden_second_grad, normed_second, inv_second, gain_second
    )
    residual_grad_low = residual_grad.astype(bf16)
    grad_proj_bias = jnp.sum(residual_grad, axis=0)
    attended_grad = dot(residual_grad_low, proj_full, 1, 1).astype(bf16)
    attended_grad = attended_grad.reshape(items, tokens, ranks, 2, head_cols)
    mine = by_core(
        pick(attended_grad, core, 3), swap(pick(attended_grad, 1 - core, 3)), 0
    ).reshape(column_items, tokens, ranks, head_cols)
    mine = jnp.moveaxis(mine, 2, 1).reshape(seq_ways, tokens, head_cols)
    grad_heads = lax.all_to_all(mine, "seq", 0, 0).reshape(length, head_cols)

    grad_fc_two = dot(acts, cotangent_all, 0, 0).astype(bf16)
    grad_fc_one = dot(hidden_second, pre_grad_low, 0, 0).astype(bf16)
    grad_proj = dot(attended_rows, residual_grad_low, 0, 0).astype(bf16)

    def shares(vector):
        return vector.reshape(dp_ways, -1)

    one_parts = grad_bias_one.reshape(chips, 1, -1)
    one_all = jnp.where(
        jnp.arange(2)[None, :, None] == core, jnp.broadcast_to(one_parts, (chips, 2, one_parts.shape[2])), 0.0
    )
    extra = jnp.concatenate(
        [
            shares(grad_proj_bias),
            shares(grad_gain_second),
            shares(grad_shift_second),
            shares(grad_bias_two),
            shares(one_all),
        ],
        axis=1,
    ).astype(bf16)
    extra = jnp.pad(extra[:, None, :], ((0, 0), (0, 15), (0, width - extra.shape[1])))
    proj_blocks = jnp.concatenate([grad_proj.reshape(dp_ways, shard_rows, width), extra], axis=1)

    share_two = scatter_chips(grad_fc_two.reshape(chips, -1, width))
    share_one = scatter_chips(grad_fc_one.reshape(chips, 2 * shard_rows, -1))
    share_proj = lax.psum_scatter(proj_blocks, "dp", scatter_dimension=0, tiled=True)[0]
    share_two = lax.psum(share_two, "seq")
    share_one, share_two = lax.optimization_barrier((share_one, share_two))
    share_one = lax.psum(share_one, "seq")
    share_proj, share_one = lax.optimization_barrier((share_proj, share_one))
    share_proj = lax.psum(share_proj, "seq")

    qkv_grad, bias_sums = attend_back(projected, attended, log_total, grad_heads)
    hidden_partial = dot(qkv_grad, qkv_full, 1, 1)
    grad_gain_first = jnp.sum(hidden_partial * normed_image, axis=0)
    grad_shift_first = jnp.sum(hidden_partial, axis=0)
    partial_parts = hidden_partial.reshape(seq_ways, 2, half, width)
    chip_sum = pick(partial_parts, core, 1) + swap(
        pick(partial_parts, 1 - core, 1).astype(bf16)
    ).astype(f32)
    home = lax.all_to_all(chip_sum.astype(bf16), "seq", 0, 0)
    home = home.reshape(2, items, ranks, half, width)
    if ranks > 1:
        home = jnp.sum(home.astype(f32), axis=2, keepdims=True).astype(bf16)
    home = home[:, :, 0]
    hidden_first_grad = by_core(pick(home, core, 0), swap(pick(home, 1 - core, 0)), 1)
    hidden_first_grad = hidden_first_grad.reshape(own_rows, width).astype(f32)
    normed_first, inv_first = norm_stats(flat_rows)
    image_grad = residual_grad + norm_backward(
        hidden_first_grad, normed_first, inv_first, gain_first
    )

    grad_qkv = dot(hidden_first, qkv_grad, 0, 0).astype(bf16)
    grad_qkv = grad_qkv.reshape(chips, 2 * shard_rows, 3, 1, head_cols)
    qv_sums = jnp.moveaxis(bias_sums, 1, 0).reshape(2, 1, head_cols)
    qv_all = lax.dynamic_update_slice(jnp.zeros((2, groups, head_cols), f32), qv_sums, (0, group, 0))
    extra = jnp.concatenate(
        [
            grad_gain_first.reshape(chips, -1),
            grad_shift_first.reshape(chips, -1),
            qv_all.reshape(chips, -1),
        ],
        axis=1,
    ).astype(bf16)
    extra_cols = extra.shape[1]
    extra = jnp.pad(extra[:, None, :], ((0, 0), (0, 15), (0, 3 * head_cols - extra_cols)))
    blocks = jnp.concatenate(
        [grad_qkv.reshape(chips, 2 * shard_rows, 3 * head_cols), extra], axis=1
    )
    share_qkv = scatter_chips(blocks)
    extra = share_qkv[2 * shard_rows, :extra_cols]
    share_qkv = share_qkv[: 2 * shard_rows].reshape(2 * shard_rows, 3, 1, head_cols)
    if ranks > 1:
        share_qkv = lax.dynamic_update_slice(
            jnp.zeros((2 * shard_rows, 3, ranks, head_cols), bf16), share_qkv, (0, 0, rank, 0)
        )
    flat = jnp.concatenate(
        [
            share_qkv.reshape(2 * shard_rows, -1),
            jnp.pad(extra[None], ((0, 15), (0, ranks * 3 * head_cols - extra_cols))),
        ],
        axis=0,
    )
    flat, share_proj = lax.optimization_barrier((flat, share_proj))
    flat = lax.psum(flat, "seq")
    rows_parts = flat[: 2 * shard_rows].reshape(2, shard_rows, 3, ranks, head_cols)
    extra = flat[2 * shard_rows : 2 * shard_rows + 1]
    out_qkv = by_core(pick(rows_parts, core, 0), swap(pick(rows_parts, 1 - core, 0)), 3)
    out_qkv = out_qkv.reshape(shard_rows, 3 * width).astype(f32)
    extra = (extra.astype(f32) + swap(extra).astype(f32))[0]
    per_chip = width // chips
    out_gain_first = pick(extra[:per_chip].reshape(2, -1), core, 0)
    out_shift_first = pick(extra[per_chip : 2 * per_chip].reshape(2, -1), core, 0)
    out_qv = pick(extra[2 * per_chip : 4 * per_chip].reshape(2, -1), core, 0)

    one_rows = share_one.reshape(2, shard_rows, chips, -1)
    out_one = by_core(pick(one_rows, core, 0), swap(pick(one_rows, 1 - core, 0)), 2)
    out_one = out_one.reshape(shard_rows, -1).astype(f32)
    last = share_proj[shard_rows].astype(f32)
    out_smalls, at = [], 0
    for size in (shard_rows, shard_rows, shard_rows, shard_rows, 4 * shard_rows):
        out_smalls.append(last[at : at + size])
        at += size
    return (
        output.reshape(images.shape),
        image_grad.reshape(images.shape),
        out_qkv,
        out_qv,
        share_proj[:shard_rows].astype(f32),
        out_smalls[0],
        out_gain_first,
        out_shift_first,
        out_smalls[1],
        out_smalls[2],
        out_one,
        out_smalls[4],
        share_two.astype(f32),
        out_smalls[3],
    )


def solution(mesh):
    rows, cols, flat = P("dp", "seq", None), P("dp", None), P("dp")
    in_specs = (rows, cols, flat, cols, flat, flat, flat, flat, flat, cols, flat, cols, flat, rows)
    out_specs = (rows, rows, cols, flat, cols, flat, flat, flat, flat, flat, cols, flat, cols, flat)
    return jax.shard_map(body, mesh=mesh, in_specs=in_specs, out_specs=out_specs, check_vma=False)
```

```python
import functools

import jax
import jax.numpy as jnp
from jax import lax
from jax.experimental import pallas as pl
from jax.experimental.pallas import tpu as pltpu
from jax.sharding import PartitionSpec as P

HEAD_DIM = 64
LANES = 128
f32 = jnp.float32
bf16 = jnp.bfloat16

epsilon = 1e-06


def norm_stats(matrix):
    mean_val = jnp.mean(matrix, axis=-1, keepdims=True)
    centred = matrix - mean_val
    inv_std = lax.rsqrt(jnp.mean(centred * centred, axis=-1, keepdims=True) + epsilon)
    return (centred * inv_std, inv_std)


def norm_backward(grad_in, normed, inv_std, gain):
    scaled = grad_in * gain
    return inv_std * (
        scaled
        - jnp.mean(scaled, axis=-1, keepdims=True)
        - normed * jnp.mean(scaled * normed, axis=-1, keepdims=True)
    )


def gelu_cdf(pre_act):
    return 0.5 * (1.0 + lax.erf(pre_act * 0.7071067811865476))


def gelu_slope(pre_act):
    return gelu_cdf(pre_act) + pre_act * jnp.exp(-0.5 * pre_act * pre_act) * 0.3989422804014327


def dot(left, right, left_dim=1, right_dim=0):
    return lax.dot_general(
        left, right, (((left_dim,), (right_dim,)), ((), ())), preferred_element_type=f32
    )


def transpose_low(matrix):
    return matrix.astype(f32).T.astype(bf16)


def pair_masks():
    lane = lax.broadcasted_iota(jnp.int32, (1, LANES), 1)
    return (lane < HEAD_DIM, lane >= HEAD_DIM)


def attend_kernel(q_ref, k_ref, v_ref, out_ref, lse_ref, v_flip):
    @pl.when(pl.program_id(1) == 0)
    def _():
        v_flip[...] = transpose_low(v_ref[...])

    query = q_ref[...] * jnp.asarray(HEAD_DIM**-0.5, bf16)
    key = k_ref[...]
    pieces = []
    for head, mask in enumerate(pair_masks()):
        scores = dot(key, jnp.where(mask, query, jnp.zeros_like(query)), 1, 1)
        peak = jnp.max(scores, axis=0, keepdims=True)
        lifted = jnp.exp(scores - peak)
        total = jnp.sum(lifted, axis=0, keepdims=True)
        probs = (lifted * (1.0 / total)).astype(bf16)
        rows = slice(head * HEAD_DIM, (head + 1) * HEAD_DIM)
        pieces.append(dot(v_flip[rows, :], probs))
        lse_ref[0, head : head + 1, :] = peak + jnp.log(total)
    out_ref[...] = jnp.concatenate(pieces, axis=0).T.astype(bf16)


def attend_back_kernel(
    q_ref, k_ref, v_ref, out_ref, grad_ref, lse_ref, all_ref, sums_ref, k_flip, dk_sum, dv_sum
):
    pair, block = pl.program_id(0), pl.program_id(1)
    pairs, blocks = pl.num_programs(0), pl.num_programs(1)
    block_rows = q_ref.shape[0]

    @pl.when(block == 0)
    def _():
        k_flip[...] = transpose_low(k_ref[...])
        dk_sum[...] = jnp.zeros_like(dk_sum)
        dv_sum[...] = jnp.zeros_like(dv_sum)
        sums_ref[...] = jnp.zeros_like(sums_ref)

    query = q_ref[...] * jnp.asarray(HEAD_DIM**-0.5, bf16)
    key = k_ref[...]
    value = v_ref[...]
    grad = grad_ref[...]
    mixed = (grad.astype(f32) * out_ref[...].astype(f32)).T
    pieces = []
    for head, mask in enumerate(pair_masks()):
        rows = slice(head * HEAD_DIM, (head + 1) * HEAD_DIM)
        query_one = jnp.where(mask, query, jnp.zeros_like(query))
        grad_one = jnp.where(mask, grad, jnp.zeros_like(grad))
        probs = jnp.exp(dot(key, query_one, 1, 1) - lse_ref[0, head : head + 1, :])
        prob_grad = dot(value, grad_one, 1, 1)
        delta = jnp.sum(mixed[rows], axis=0, keepdims=True)
        score_grad = (probs * (prob_grad - delta) * HEAD_DIM**-0.5).astype(bf16)
        dv_sum[...] += dot(probs.astype(bf16), grad_one)
        dk_sum[...] += dot(score_grad, query_one)
        pieces.append(dot(k_flip[rows, :], score_grad))
    query_grad = jnp.concatenate(pieces, axis=0).T
    row_at = pl.multiple_of(block * block_rows, block_rows)
    lanes = pl.ds(pl.multiple_of(pair * LANES, LANES), LANES)
    all_ref[pl.ds(row_at, block_rows), lanes] = query_grad.astype(bf16)
    sums_ref[0, 0:1, :] += jnp.sum(query_grad, axis=0, keepdims=True)

    @pl.when(block == blocks - 1)
    def _():
        key_lanes = pl.ds(pl.multiple_of((pairs + pair) * LANES, LANES), LANES)
        value_lanes = pl.ds(pl.multiple_of((2 * pairs + pair) * LANES, LANES), LANES)
        all_ref[:, key_lanes] = (dk_sum[...] * HEAD_DIM**0.5).astype(bf16)
        all_ref[:, value_lanes] = dv_sum[...].astype(bf16)
        sums_ref[0, 1:2, :] = jnp.sum(dv_sum[...], axis=0, keepdims=True)


def block_size(length):
    return next(
        size
        for size in (384, 256, 128, length)
        if length % size == 0 and (size * length <= 384 * 1152 or size <= 128 or size == length)
    )


def attend(projected):
    length, head_cols = projected.shape[0], projected.shape[1] // 3
    pairs = head_cols // LANES
    rows = block_size(length)
    query_spec = pl.BlockSpec((rows, LANES), lambda h, b: (b, h))
    return pl.pallas_call(
        attend_kernel,
        grid=(pairs, length // rows),
        in_specs=[
            query_spec,
            pl.BlockSpec((length, LANES), lambda h, b: (0, pairs + h)),
            pl.BlockSpec((length, LANES), lambda h, b: (0, 2 * pairs + h)),
        ],
        out_specs=[query_spec, pl.BlockSpec((1, 2, rows), lambda h, b: (h, 0, b))],
        out_shape=[
            jax.ShapeDtypeStruct((length, head_cols), bf16),
            jax.ShapeDtypeStruct((pairs, 2, length), f32),
        ],
        scratch_shapes=[pltpu.VMEM((LANES, length), bf16)],
        compiler_params=pltpu.CompilerParams(vmem_limit_bytes=58 * 2**20),
        cost_estimate=pl.CostEstimate(
            flops=16 * pairs * length * length * LANES,
            bytes_accessed=8 * length * head_cols,
            transcendentals=2 * pairs * length * length,
        ),
        name="attend",
    )(projected, projected, projected)


def attend_back(projected, attended, log_total, grad):
    length, head_cols = attended.shape
    pairs = head_cols // LANES
    rows = block_size(length)
    query_spec = pl.BlockSpec((rows, LANES), lambda h, b: (b, h))
    return pl.pallas_call(
        attend_back_kernel,
        grid=(pairs, length // rows),
        in_specs=[
            query_spec,
            pl.BlockSpec((length, LANES), lambda h, b: (0, pairs + h)),
            pl.BlockSpec((length, LANES), lambda h, b: (0, 2 * pairs + h)),
            query_spec,
            query_spec,
            pl.BlockSpec((1, 2, rows), lambda h, b: (h, 0, b)),
        ],
        out_specs=[
            pl.BlockSpec((length, 3 * head_cols), lambda h, b: (0, 0)),
            pl.BlockSpec((1, 2, LANES), lambda h, b: (h, 0, 0)),
        ],
        out_shape=[
            jax.ShapeDtypeStruct((length, 3 * head_cols), bf16),
            jax.ShapeDtypeStruct((pairs, 2, LANES), f32),
        ],
        scratch_shapes=[
            pltpu.VMEM((LANES, length), bf16),
            pltpu.VMEM((length, LANES), f32),
            pltpu.VMEM((length, LANES), f32),
        ],
        compiler_params=pltpu.CompilerParams(vmem_limit_bytes=58 * 2**20),
        cost_estimate=pl.CostEstimate(
            flops=40 * pairs * length * length * LANES,
            bytes_accessed=16 * length * head_cols,
            transcendentals=2 * pairs * length * length,
        ),
        name="attend_back",
    )(projected, projected, projected, attended, grad, log_total)


class Copies:
    def __init__(self, send_sems, recv_sems, local_sems):
        self.send_sems, self.recv_sems, self.local_sems = send_sems, recv_sems, local_sems
        self.sent, self.locals, self.local_count = [], [], 0

    def remote(self, src, dst, **device):
        at = len(self.sent)
        copy = pltpu.make_async_remote_copy(
            src_ref=src,
            dst_ref=dst,
            send_sem=self.send_sems.at[at],
            recv_sem=self.recv_sems.at[at],
            device_id=device,
            device_id_type=pl.DeviceIdType.MESH,
        )
        copy.start()
        self.sent.append(copy)
        return copy

    def local(self, src, dst):
        copy = pltpu.make_async_copy(src, dst, self.local_sems.at[self.local_count])
        copy.start()
        self.locals.append(copy)
        self.local_count += 1
        return copy

    def wait_local(self, copy):
        copy.wait()
        self.locals = [kept for kept in self.locals if kept is not copy]

    def finish(self):
        for copy in self.sent:
            copy.wait_send()
        for copy in self.locals:
            copy.wait()


class Place:
    def __init__(self, items):
        self.dp_ways, self.seq_ways = lax.axis_size("dp"), lax.axis_size("seq")
        self.chips = self.dp_ways // 2
        self.ranks = self.seq_ways // (2 * items)
        self.dp, self.seq = lax.axis_index("dp"), lax.axis_index("seq")
        self.core, self.chip = lax.rem(self.dp, 2), lax.div(self.dp, 2)
        self.rank = lax.rem(self.seq, self.ranks)
        self.item = lax.div(self.seq, self.ranks)

    def partner(self, offset):
        if self.chips == 4:
            x, y = lax.rem(self.chip, 2), lax.div(self.chip, 2)
            x = 1 - x if offset % 2 else x
            y = 1 - y if offset >= 2 else y
            return y * 2 + x
        return lax.rem(self.chip + offset, self.chips)

    def source(self, offset):
        if self.chips == 4:
            return self.partner(offset)
        return lax.rem(self.chip + self.chips - offset, self.chips)

    def meet(self):
        barrier = pltpu.get_barrier_semaphore()
        for step in range(1, self.dp_ways):
            pl.semaphore_signal(
                barrier,
                inc=1,
                device_id={"dp": lax.rem(self.dp + step, self.dp_ways)},
                device_id_type=pl.DeviceIdType.MESH,
            )
        for step in range(1, self.seq_ways):
            for core in range(2):
                pl.semaphore_signal(
                    barrier,
                    inc=1,
                    device_id={
                        "dp": self.chip * 2 + core,
                        "seq": lax.rem(self.seq + step, self.seq_ways),
                    },
                    device_id_type=pl.DeviceIdType.MESH,
                )
        pl.semaphore_wait(barrier, self.dp_ways - 1 + 2 * (self.seq_ways - 1))


def rows_at(start, size):
    return pl.ds(pl.multiple_of(start, 16), size)


def lanes_at(start, size):
    return pl.ds(pl.multiple_of(start, LANES), size)


def attend_rows(prj, out, lse, v_flip, pair, block, rows):
    pairs = out.shape[1] // LANES
    query = prj[rows_at(block * rows, rows), lanes_at(pair * LANES, LANES)]
    query = query * jnp.asarray(HEAD_DIM**-0.5, bf16)
    key = prj[:, lanes_at((pairs + pair) * LANES, LANES)]
    pieces = []
    for head, mask in enumerate(pair_masks()):
        scores = dot(key, jnp.where(mask, query, jnp.zeros_like(query)), 1, 1)
        peak = jnp.max(scores, axis=0, keepdims=True)
        lifted = jnp.exp(scores - peak)
        total = jnp.sum(lifted, axis=0, keepdims=True)
        probs = (lifted * (1.0 / total)).astype(bf16)
        pieces.append(dot(v_flip[head * HEAD_DIM : (head + 1) * HEAD_DIM, :], probs))
        lse[pair, head : head + 1, lanes_at(block * rows, rows)] = peak + jnp.log(total)
    out[rows_at(block * rows, rows), lanes_at(pair * LANES, LANES)] = (
        jnp.concatenate(pieces, axis=0).T.astype(bf16)
    )


def forward_kernel(
    items,
    img,
    wq,
    wp,
    w1,
    w2,
    cot,
    small,
    img_out,
    wq_out,
    wp_out,
    w1_out,
    w2_out,
    cot_out,
    small_out,
    prj_out,
    heads_out,
    lse_out,
    rows_out,
    img_v,
    wq_v,
    prj_v,
    heads_v,
    small_v,
    vec_v,
    v_flip,
    send_sems,
    recv_sems,
    local_sems,
    swap_sems,
    token_send,
    token_recv,
    back_send,
    back_recv,
):
    at = Place(items)
    chips, ranks, seq_ways, dp_ways = at.chips, at.ranks, at.seq_ways, at.dp_ways
    tokens = img.shape[0] // items
    half = tokens // 2
    shard, width = wp.shape
    head_cols = heads_v.shape[1]
    unit_rows = w2.shape[0]
    length = img_v.shape[0]
    pairs = head_cols // LANES
    relay = chips == 4
    offsets = (1, 2) if relay else tuple(range(1, chips))
    copies = Copies(send_sems, recv_sems, local_sems)
    at.meet()
    me = rows_at(at.dp * shard, shard)

    token_jobs = []
    for item in range(items):
        for k in range(ranks):
            for h in range(2):
                to_seq = (at.core * items + item) * ranks + k
                mine = (to_seq == at.seq) & (at.core == h)
                src = img.at[pl.ds(item * tokens + h * half, half), :]
                dst = img_v.at[rows_at(at.seq * tokens + h * half, half), :]
                sem = token_send.at[len(token_jobs)]
                far = pltpu.make_async_remote_copy(
                    src_ref=src,
                    dst_ref=dst,
                    send_sem=sem,
                    recv_sem=token_recv.at[at.seq],
                    device_id={"dp": at.chip * 2 + h, "seq": to_seq},
                    device_id_type=pl.DeviceIdType.MESH,
                )
                near = pltpu.make_async_copy(src, dst, token_recv.at[at.seq])
                pl.when(mine)(near.start)
                pl.when(jnp.logical_not(mine))(far.start)
                token_jobs.append((mine, far))

    other = at.chip * 2 + 1 - at.core
    small_copies = []
    small_rows = pl.ds(pl.multiple_of(at.dp * 8, 8), 8)
    small_own = copies.local(small, small_v.at[small_rows, :])
    for step in range(1, dp_ways):
        small_copies.append(
            copies.remote(small, small_v.at[small_rows, :], dp=lax.rem(at.dp + step, dp_ways))
        )

    def qkv_pieces(core):
        group = at.rank * 2 + core
        return [
            (
                wq.at[:, lanes_at(part * width + group * head_cols, head_cols)],
                wq_v.at[me, pl.ds(part * head_cols, head_cols)],
            )
            for part in range(3)
        ]

    def fc1_pieces(core):
        return [
            (
                w1.at[:, lanes_at((2 * q + core) * unit_rows, unit_rows)],
                w1_out.at[me, pl.ds(q * unit_rows, unit_rows)],
            )
            for q in range(chips)
        ]

    def start_columns(pieces):
        arrivals = {0: [], "local": [copies.local(src, dst) for src, dst in pieces(at.core)]}
        for src, dst in pieces(1 - at.core):
            arrivals[0].append(copies.remote(src, dst, dp=other))
        for offset in offsets:
            for core in (at.core, 1 - at.core):
                for src, dst in pieces(core):
                    copy = copies.remote(src, dst, dp=at.partner(offset) * 2 + core)
                    arrivals.setdefault(offset, []).append(copy)
        return arrivals

    def pass_on(arrivals, block_of, first, second):
        for copy in arrivals[1]:
            copy.wait_recv()
        last = []
        if relay:
            ref = block_of(at.partner(1), *first)
            last.append(copies.remote(ref, ref, dp=at.partner(2) * 2 + at.core))
        for copy in arrivals[2]:
            copy.wait_recv()
        if relay:
            ref = block_of(at.partner(2), *second)
            last.append(copies.remote(ref, ref, dp=at.partner(1) * 2 + at.core))
        for offset in range(3, chips):
            if not relay:
                for copy in arrivals[offset]:
                    copy.wait_recv()
        return last

    def settle(arrivals, last):
        for copy in last:
            copy.wait_recv()
        for copy in arrivals[0]:
            copy.wait_recv()

    def shard_halves(ref):
        return lambda chip, start, size: ref.at[rows_at(chip * 2 * shard + start, size), :]

    qkv_arrivals = start_columns(qkv_pieces)

    wp_near = [copies.remote(wp, wp_out.at[me, :], dp=other)]
    copies.local(wp, wp_out.at[me, :])
    wp_far = {
        o: [copies.remote(wp, wp_out.at[me, :], dp=at.partner(o) * 2 + at.core)] for o in offsets
    }
    cot_rows = rows_at(at.core * cot.shape[0], cot.shape[0])
    cot_near = copies.remote(cot, cot_out.at[cot_rows, :], dp=other)
    copies.local(cot, cot_out.at[cot_rows, :])

    for s in range(seq_ways):
        pltpu.make_async_copy(
            img.at[pl.ds(0, half), :], img_v.at[pl.ds(s * tokens, half), :], token_recv.at[s]
        ).wait()
    for mine, far in token_jobs:
        pl.when(jnp.logical_not(mine))(far.wait_send)
    token_near = []
    for s in range(seq_ways):
        ref = img_v.at[rows_at(s * tokens + at.core * half, half), :]
        token_near.append(copies.remote(ref, ref, dp=other))
    qkv_last = pass_on(qkv_arrivals, shard_halves(wq_v), (0, shard), (shard, shard))
    fc1_arrivals = start_columns(fc1_pieces)
    w2_to = lambda chip: w2_out.at[rows_at(chip * unit_rows, unit_rows), :]
    copies.local(w2, w2_to(at.chip))
    fc2_arrivals = {0: []}
    for offset in offsets:
        fc2_arrivals[offset] = [
            copies.remote(w2, w2_to(at.chip), dp=at.partner(offset) * 2 + at.core)
        ]

    for copy in small_copies:
        copy.wait_recv()
    copies.wait_local(small_own)
    names = {"query": (0, 2), "gain": (3, 1), "shift": (4, 1)}
    for row, (start, size) in enumerate(names.values()):
        for i in range(dp_ways):
            vec_v[row : row + 1, i * size * shard : (i + 1) * size * shard] = small_v[
                8 * i : 8 * i + 1, start * shard : (start + size) * shard
            ]
    for copy in token_near:
        copy.wait_recv()
    settle(qkv_arrivals, qkv_last)
    for copy in qkv_arrivals["local"]:
        copies.wait_local(copy)

    group = at.rank * 2 + at.core
    gain = vec_v[1:2, :width]
    shift = vec_v[2:3, :width]

    def project(step, carry):
        rows = rows_at(step * tokens, tokens)
        normed, _ = norm_stats(img_v[rows, :].astype(f32))
        hidden = (normed * gain + shift).astype(bf16)
        for part in range(3):
            cols = slice(part * head_cols, (part + 1) * head_cols)
            block = dot(hidden, wq_v[:, cols])
            if part != 1:
                lanes = lanes_at((part // 2) * width + group * head_cols, head_cols)
                block = block + vec_v[0:1, lanes]
            prj_v[rows, cols] = block.astype(bf16)
        return carry

    lax.fori_loop(0, seq_ways, project, 0)
    copies.local(img_v, img_out)
    copies.local(wq_v, wq_out)
    copies.local(prj_v, prj_out)
    copies.local(small_v, small_out)

    rows = block_size(length)
    home_core = lax.div(at.item, items)
    home_item = lax.rem(at.item, items)

    def back_copies(pair):
        jobs = []
        for s in range(seq_ways):
            mine = (at.seq == s) & (at.core == home_core)
            src = heads_v.at[pl.ds(s * tokens, tokens), lanes_at(pair * LANES, LANES)]
            dst = rows_out.at[
                rows_at(home_item * tokens, tokens),
                lanes_at(group * head_cols + pair * LANES, LANES),
            ]
            far = pltpu.make_async_remote_copy(
                src_ref=src,
                dst_ref=dst,
                send_sem=back_send.at[pair, s],
                recv_sem=back_recv,
                device_id={"dp": at.chip * 2 + home_core, "seq": s},
                device_id_type=pl.DeviceIdType.MESH,
            )
            near = pltpu.make_async_copy(src, dst, back_recv)
            jobs.append((mine, far, near))
        return jobs

    def one_pair(pair, carry):
        v_flip[...] = transpose_low(prj_v[:, lanes_at((2 * pairs + pair) * LANES, LANES)])

        def one_block(block, inner):
            attend_rows(prj_v, heads_v, lse_out, v_flip, pair, block, rows)
            return inner

        lax.fori_loop(0, length // rows, one_block, 0)
        for mine, far, near in back_copies(pair):
            pl.when(mine)(near.start)
            pl.when(jnp.logical_not(mine))(far.start)
        return carry

    lax.fori_loop(0, pairs, one_pair, 0)
    copies.local(heads_v, heads_out)
    wp_last = pass_on(
        wp_far,
        lambda chip, start, size: wp_out.at[
            rows_at((chip * 2 + at.core) * shard + start, size), :
        ],
        (0, shard // 2),
        (shard // 2, shard // 2),
    )
    fc1_last = pass_on(fc1_arrivals, shard_halves(w1_out), (0, shard), (shard, shard))
    for copy in wp_last:
        copy.wait_recv()
    for offset in range(1, chips):
        ref = wp_out.at[rows_at((at.source(offset) * 2 + at.core) * shard, shard), :]
        wp_near.append(copies.remote(ref, ref, dp=other))
    fc2_last = pass_on(
        fc2_arrivals,
        lambda chip, start, size: w2_out.at[rows_at(chip * unit_rows + start, size), :],
        (0, unit_rows // 2),
        (unit_rows // 2, unit_rows // 2),
    )
    settle(fc1_arrivals, fc1_last)
    settle(fc2_arrivals, fc2_last)
    for copy in wp_near:
        copy.wait_recv()
    cot_near.wait_recv()
    pltpu.make_async_copy(rows_out, rows_out, back_recv).wait()

    def drain(pair, carry):
        for mine, far, _ in back_copies(pair):
            pl.when(jnp.logical_not(mine))(far.wait_send)
        return carry

    lax.fori_loop(0, pairs, drain, 0)
    copies.finish()


def forward(items, img, wq, wp, w1, w2, cot, small):
    dp_ways, seq_ways = lax.axis_size("dp"), lax.axis_size("seq")
    ranks = seq_ways // (2 * items)
    shard, width = wp.shape
    head_cols = width // (2 * ranks)
    tokens = img.shape[0] // items
    length = seq_ways * tokens
    half_units = w1.shape[1] // 2
    pairs = head_cols // LANES
    any_spec = pl.BlockSpec(memory_space=pl.ANY)
    out_shape = [
        jax.ShapeDtypeStruct((length, width), bf16),
        jax.ShapeDtypeStruct((width, 3 * head_cols), bf16),
        jax.ShapeDtypeStruct((width, width), bf16),
        jax.ShapeDtypeStruct((width, half_units), bf16),
        jax.ShapeDtypeStruct((half_units, width), bf16),
        jax.ShapeDtypeStruct((2 * cot.shape[0], width), bf16),
        jax.ShapeDtypeStruct((8 * dp_ways, small.shape[1]), f32),
        jax.ShapeDtypeStruct((length, 3 * head_cols), bf16),
        jax.ShapeDtypeStruct((length, head_cols), bf16),
        jax.ShapeDtypeStruct((pairs, 2, length), f32),
        jax.ShapeDtypeStruct(img.shape, bf16),
    ]
    out_specs = [any_spec] * len(out_shape)
    out_specs[9] = pl.BlockSpec(memory_space=pltpu.VMEM)
    remotes = 160
    return pl.pallas_call(
        functools.partial(forward_kernel, items),
        in_specs=[any_spec] * 7,
        out_specs=out_specs,
        out_shape=out_shape,
        scratch_shapes=[
            pltpu.VMEM((length, width), bf16),
            pltpu.VMEM((width, 3 * head_cols), bf16),
            pltpu.VMEM((length, 3 * head_cols), bf16),
            pltpu.VMEM((length, head_cols), bf16),
            pltpu.VMEM((8 * dp_ways, small.shape[1]), f32),
            pltpu.VMEM((8, 2 * width), f32),
            pltpu.VMEM((LANES, length), bf16),
            pltpu.SemaphoreType.DMA((remotes,)),
            pltpu.SemaphoreType.DMA((remotes,)),
            pltpu.SemaphoreType.DMA((32,)),
            pltpu.SemaphoreType.DMA((2,)),
            pltpu.SemaphoreType.DMA((2 * items * ranks,)),
            pltpu.SemaphoreType.DMA((seq_ways,)),
            pltpu.SemaphoreType.DMA((pairs, seq_ways)),
            pltpu.SemaphoreType.DMA,
        ],
        compiler_params=pltpu.CompilerParams(
            collective_id=0, has_side_effects=True, vmem_limit_bytes=62 * 2**20
        ),
        name="forward",
    )(img, wq, wp, w1, w2, cot, small)


class Share:
    def __init__(self, at, copies, slots, total, line, final):
        self.at, self.copies = at, copies
        self.slots, self.total, self.line, self.final = slots, total, line, final
        self.part = total.shape[0] // at.seq_ways

    def spread(self, block_of):
        at = self.at
        self.arrivals = [
            self.copies.remote(
                block_of(at.partner(offset)),
                self.slots.at[offset - 1],
                dp=at.partner(offset) * 2 + at.core,
            )
            for offset in range(1, at.chips)
        ]

    def add_chips(self):
        for copy in self.arrivals:
            copy.wait_recv()
        step = 64 if self.total.shape[0] % 64 == 0 else 16

        def add(i, carry):
            rows = rows_at(i * step, step)
            value = self.total[rows, :].astype(f32)
            for slot in range(self.at.chips - 1):
                value = value + self.slots[slot, rows, :].astype(f32)
            self.total[rows, :] = value.astype(bf16)
            return carry

        lax.fori_loop(0, self.total.shape[0] // step, add, 0)
        self.arrivals = []
        for step in range(1, self.at.seq_ways):
            to = lax.rem(self.at.seq + step, self.at.seq_ways)
            self.arrivals.append(
                self.copies.remote(
                    self.total.at[rows_at(to * self.part, self.part), :],
                    self.line.at[step - 1],
                    seq=to,
                )
            )

    def add_line(self):
        for copy in self.arrivals:
            copy.wait_recv()
        rows = rows_at(self.at.seq * self.part, self.part)
        value = self.total[rows, :].astype(f32)
        for slot in range(self.at.seq_ways - 1):
            value = value + self.line[slot].astype(f32)
        self.final[rows, :] = value.astype(bf16)
        self.arrivals = []
        for step in range(1, self.at.seq_ways):
            to = lax.rem(self.at.seq + step, self.at.seq_ways)
            self.arrivals.append(
                self.copies.remote(self.final.at[rows, :], self.final.at[rows, :], seq=to)
            )

    def arrive(self):
        for copy in self.arrivals:
            copy.wait_recv()


def backward_kernel(
    items,
    rgl,
    wp,
    g2,
    g1,
    gp,
    prj,
    heads,
    img,
    wq,
    small,
    lse,
    home_out,
    o2_out,
    op_out,
    o1_out,
    oq_out,
    ox_out,
    rgl_v,
    wp_v,
    prj_v,
    heads_v,
    img_v,
    wq_v,
    small_v,
    da_v,
    do_v,
    hid_v,
    dqkv_v,
    keep_v,
    near_v,
    vec_v,
    k_flip,
    dk_sum,
    dv_sum,
    slots2,
    total2,
    line2,
    final2,
    slots1,
    total1,
    line1,
    final1,
    pair_own,
    pair_far,
    slotsp,
    totalp,
    linep,
    finalp,
    gq_v,
    slotsq,
    totalq,
    lineq,
    finalq,
    swap1,
    swapq,
    swapx,
    send_sems,
    recv_sems,
    local_sems,
    token_send,
    token_recv,
    home_send,
    home_recv,
):
    at = Place(items)
    chips, ranks, seq_ways = at.chips, at.ranks, at.seq_ways
    own_rows, width = rgl.shape
    tokens = own_rows // items
    half = tokens // 2
    shard = width // at.dp_ways
    head_cols = heads.shape[1]
    length = heads.shape[0]
    pairs = head_cols // LANES
    unit_rows = total2.shape[0]
    copies = Copies(send_sems, recv_sems, local_sems)
    at.meet()
    other = at.chip * 2 + 1 - at.core
    group = at.rank * 2 + at.core

    first_loads = [copies.local(rgl, rgl_v.at[pl.ds(0, own_rows), :]), copies.local(wp, wp_v)]
    share2 = Share(at, copies, slots2, total2, line2, final2)
    share1 = Share(at, copies, slots1, total1, line1, final1)
    sharep = Share(at, copies, slotsp, totalp, linep, finalp)
    shareq = Share(at, copies, slotsq, totalq, lineq, finalq)
    pair_rows = pair_own.shape[0]
    pair_copy = copies.remote(gp.at[rows_at((1 - at.core) * pair_rows, pair_rows), :], pair_far, dp=other)
    pair_load = copies.local(gp.at[rows_at(at.core * pair_rows, pair_rows), :], pair_own)

    def block2(chip):
        return g2.at[rows_at(chip * unit_rows, unit_rows), :]

    def block1(chip):
        return g1.at[rows_at(chip * 2 * shard, 2 * shard), :]

    share2.spread(block2)
    share1.spread(block1)
    load2 = copies.local(block2(at.chip), total2)
    load1 = copies.local(block1(at.chip), total1)
    hidden_loads = [copies.local(img, img_v), copies.local(small, small_v)]
    loads = [copies.local(prj, prj_v), copies.local(heads, heads_v), copies.local(wq, wq_v)]

    for copy in first_loads:
        copies.wait_local(copy)
    jobs = []
    for item in range(items):
        rows = pl.ds(item * tokens, tokens)
        da_v[rows, :] = dot(rgl_v[rows, :], wp_v[...], 1, 1).astype(bf16)
        for k in range(ranks):
            for h in range(2):
                to_seq = (at.core * items + item) * ranks + k
                mine = (to_seq == at.seq) & (at.core == h)
                src = da_v.at[rows, pl.ds((k * 2 + h) * head_cols, head_cols)]
                dst = do_v.at[rows_at(at.seq * tokens, tokens), :]
                far = pltpu.make_async_remote_copy(
                    src_ref=src,
                    dst_ref=dst,
                    send_sem=token_send.at[len(jobs)],
                    recv_sem=token_recv.at[at.seq],
                    device_id={"dp": at.chip * 2 + h, "seq": to_seq},
                    device_id_type=pl.DeviceIdType.MESH,
                )
                near = pltpu.make_async_copy(src, dst, token_recv.at[at.seq])
                pl.when(mine)(near.start)
                pl.when(jnp.logical_not(mine))(far.start)
                jobs.append((mine, far))

    pair_copy.wait_recv()
    copies.wait_local(pair_load)
    step = 64

    def add_pair(i, carry):
        rows = rows_at(i * step, step)
        pair_own[rows, :] = (pair_own[rows, :].astype(f32) + pair_far[rows, :].astype(f32)).astype(bf16)
        return carry

    lax.fori_loop(0, pair_rows // step, add_pair, 0)
    block_p = pair_rows // chips
    sharep.spread(lambda chip: pair_own.at[rows_at(chip * block_p, block_p), :])

    def own_p(i, carry):
        totalp[rows_at(i * 16, 16), :] = pair_own[rows_at(at.chip * block_p + i * 16, 16), :]
        return carry

    lax.fori_loop(0, block_p // 16, own_p, 0)

    for copy in hidden_loads:
        copies.wait_local(copy)
    for row, start in ((0, 3), (1, 4)):
        for i in range(at.dp_ways):
            vec_v[row : row + 1, i * shard : (i + 1) * shard] = small_v[
                8 * i : 8 * i + 1, start * shard : (start + 1) * shard
            ]
    gain = vec_v[0:1, :width]
    shift = vec_v[1:2, :width]

    def hide(s, carry):
        rows = rows_at(s * tokens, tokens)
        normed, _ = norm_stats(img_v[rows, :].astype(f32))
        hid_v[rows, :] = (normed * gain + shift).astype(bf16)
        return carry

    lax.fori_loop(0, seq_ways, hide, 0)
    for copy in loads:
        copies.wait_local(copy)
    for s in range(seq_ways):
        pltpu.make_async_copy(
            do_v.at[pl.ds(s * tokens, tokens), :], do_v.at[pl.ds(s * tokens, tokens), :], token_recv.at[s]
        ).wait()
    for mine, far in jobs:
        pl.when(jnp.logical_not(mine))(far.wait_send)

    rows_q = block_size(length)
    vec_v[2:4, :] = jnp.zeros((2, vec_v.shape[1]), f32)
    vec_v[4:5, :] = jnp.zeros((1, vec_v.shape[1]), f32)

    def one_pair(pair, carry):
        q_lanes = lanes_at(pair * LANES, LANES)
        k_lanes = lanes_at((pairs + pair) * LANES, LANES)
        v_lanes = lanes_at((2 * pairs + pair) * LANES, LANES)
        k_flip[...] = transpose_low(prj_v[:, k_lanes])
        dk_sum[...] = jnp.zeros_like(dk_sum)
        dv_sum[...] = jnp.zeros_like(dv_sum)

        def one_block(block, sums):
            rows = rows_at(block * rows_q, rows_q)
            query = prj_v[rows, q_lanes] * jnp.asarray(HEAD_DIM**-0.5, bf16)
            key = prj_v[:, k_lanes]
            value = prj_v[:, v_lanes]
            grad = do_v[rows, q_lanes]
            mixed = (grad.astype(f32) * heads_v[rows, q_lanes].astype(f32)).T
            pieces = []
            for head, mask in enumerate(pair_masks()):
                span = slice(head * HEAD_DIM, (head + 1) * HEAD_DIM)
                query_one = jnp.where(mask, query, jnp.zeros_like(query))
                grad_one = jnp.where(mask, grad, jnp.zeros_like(grad))
                probs = jnp.exp(dot(key, query_one, 1, 1) - lse[pair, head : head + 1, rows])
                prob_grad = dot(value, grad_one, 1, 1)
                delta = jnp.sum(mixed[span], axis=0, keepdims=True)
                score_grad = (probs * (prob_grad - delta) * HEAD_DIM**-0.5).astype(bf16)
                dv_sum[...] += dot(probs.astype(bf16), grad_one)
                dk_sum[...] += dot(score_grad, query_one)
                pieces.append(dot(k_flip[span, :], score_grad))
            query_grad = jnp.concatenate(pieces, axis=0).T
            dqkv_v[rows, q_lanes] = query_grad.astype(bf16)
            return sums + jnp.sum(query_grad, axis=0, keepdims=True)

        sums = lax.fori_loop(0, length // rows_q, one_block, jnp.zeros((1, LANES), f32))
        dqkv_v[:, k_lanes] = (dk_sum[...] * HEAD_DIM**0.5).astype(bf16)
        dqkv_v[:, v_lanes] = dv_sum[...].astype(bf16)
        vec_v[4:5, lanes_at(group * head_cols + pair * LANES, LANES)] = sums
        vec_v[4:5, lanes_at(width + group * head_cols + pair * LANES, LANES)] = jnp.sum(
            dv_sum[...], axis=0, keepdims=True
        )
        return carry

    lax.fori_loop(0, pairs // 2, one_pair, 0)
    copies.wait_local(load2)
    share2.add_chips()
    lax.fori_loop(pairs // 2, pairs, one_pair, 0)
    share2.add_line()
    sharep.add_chips()

    def widen(s, carry):
        rows = rows_at(s * tokens, tokens)
        partial = dot(dqkv_v[rows, :], wq_v[...], 1, 1)
        normed, _ = norm_stats(img_v[rows, :].astype(f32))
        vec_v[2:3, :width] += jnp.sum(partial * normed, axis=0, keepdims=True)
        vec_v[3:4, :width] += jnp.sum(partial, axis=0, keepdims=True)
        near_rows = rows_at(s * half, half)

        @pl.when(at.core == 0)
        def _():
            keep_v[near_rows, :] = partial[:half]
            da_v[near_rows, :] = partial[half:].astype(bf16)

        @pl.when(at.core == 1)
        def _():
            keep_v[near_rows, :] = partial[half:]
            da_v[near_rows, :] = partial[:half].astype(bf16)

        return carry

    lax.fori_loop(0, seq_ways, widen, 0)
    near_rows = pl.ds(0, seq_ways * half)
    near_copy = copies.remote(da_v.at[near_rows, :], near_v, dp=other)

    span = 3 * head_cols
    gq_cols = ranks * span
    per_chip = width // chips
    for q in range(chips):
        block = pl.ds(q * 2 * shard, 2 * shard)
        lanes = slice(q * 2 * shard, (q + 1) * 2 * shard)
        if ranks > 1:
            gq_v[block, :] = jnp.zeros((2 * shard, gq_v.shape[1]), bf16)
        gq_v[block, lanes_at(at.rank * span, span)] = dot(hid_v[:, lanes], dqkv_v[...], 0, 0).astype(bf16)
        rows = [vec_v[2:3, q * per_chip + i : q * per_chip + i + LANES] for i in range(0, per_chip, LANES)]
        rows += [vec_v[3:4, q * per_chip + i : q * per_chip + i + LANES] for i in range(0, per_chip, LANES)]
        rows += [
            vec_v[4:5, 2 * q * per_chip + i : 2 * q * per_chip + i + LANES]
            for i in range(0, 2 * per_chip, LANES)
        ]
        which = lax.broadcasted_iota(jnp.int32, (16, LANES), 0)
        extra = jnp.zeros((16, LANES), f32)
        for i, row in enumerate(rows):
            extra = jnp.where(which == i, row, extra)
        gq_v[pl.ds(q * 2 * shard + 16, 2 * shard - 16), gq_cols : gq_cols + LANES] = jnp.zeros(
            (2 * shard - 16, LANES), bf16
        )
        gq_v[pl.ds(q * 2 * shard, 16), gq_cols : gq_cols + LANES] = extra.astype(bf16)
    shareq.spread(lambda chip: gq_v.at[rows_at(chip * 2 * shard, 2 * shard), :])

    def own_q(i, carry):
        totalq[rows_at(i * 16, 16), :] = gq_v[rows_at(at.chip * 2 * shard + i * 16, 16), :]
        return carry

    lax.fori_loop(0, 2 * shard // 16, own_q, 0)

    near_copy.wait_recv()
    home_core = lax.div(at.item, items)
    home_item = lax.rem(at.item, items)
    home_jobs = []
    for s in range(seq_ways):
        rows = pl.ds(s * half, half)
        rgl_v[rows, :] = (keep_v[rows, :] + near_v[rows, :].astype(f32)).astype(bf16)
        mine = (at.seq == s) & (at.core == home_core)
        dst = home_out.at[
            rows_at(at.rank * own_rows + home_item * tokens + at.core * half, half), :
        ]
        far = pltpu.make_async_remote_copy(
            src_ref=rgl_v.at[rows, :],
            dst_ref=dst,
            send_sem=home_send.at[s],
            recv_sem=home_recv,
            device_id={"dp": at.chip * 2 + home_core, "seq": s},
            device_id_type=pl.DeviceIdType.MESH,
        )
        near = pltpu.make_async_copy(rgl_v.at[rows, :], dst, home_recv)
        pl.when(mine)(near.start)
        pl.when(jnp.logical_not(mine))(far.start)
        home_jobs.append((mine, far))

    sharep.add_line()
    copies.wait_local(load1)
    share1.add_chips()
    shareq.add_chips()
    share1.add_line()
    shareq.add_line()
    share2.arrive()
    copies.local(final2, o2_out)
    sharep.arrive()
    copies.local(finalp, op_out)
    share1.arrive()
    theirs = rows_at((1 - at.core) * shard, shard)
    ours = rows_at(at.core * shard, shard)
    swap1_copy = copies.remote(final1.at[theirs, :], swap1, dp=other)
    units = final1.shape[1] // chips
    for q in range(chips):
        cols = slice(q * units, (q + 1) * units)
        o1_out[:, lanes_at((2 * q + at.core) * units, units)] = final1[ours, cols]
    swap1_copy.wait_recv()
    for q in range(chips):
        cols = slice(q * units, (q + 1) * units)
        o1_out[:, lanes_at((2 * q + 1 - at.core) * units, units)] = swap1[:, cols]
    shareq.arrive()
    swapq_copy = copies.remote(final1_rows(finalq, theirs), swapq, dp=other)
    swapx_copy = copies.remote(finalq.at[pl.ds(0, 16), pl.ds(gq_cols, LANES)], swapx, dp=other)

    def place_q(ref, rows, core):
        for j in range(ranks):
            for part in range(3):
                oq_out[:, lanes_at(part * width + (j * 2 + core) * head_cols, head_cols)] = ref[
                    rows, pl.ds(j * span + part * head_cols, head_cols)
                ]

    place_q(finalq, ours, at.core)
    swapq_copy.wait_recv()
    place_q(swapq, pl.ds(0, shard), 1 - at.core)
    swapx_copy.wait_recv()
    ox_out[...] = finalq[0:16, gq_cols : gq_cols + LANES].astype(f32) + swapx[...].astype(f32)
    pltpu.make_async_copy(home_out, home_out, home_recv).wait()
    for mine, far in home_jobs:
        pl.when(jnp.logical_not(mine))(far.wait_send)
    copies.finish()


def final1_rows(ref, rows):
    return ref.at[rows, :]


def backward(items, rgl, wp, g2, g1, gp, prj, heads, img, wq, small, lse):
    dp_ways, seq_ways = lax.axis_size("dp"), lax.axis_size("seq")
    chips = dp_ways // 2
    ranks = seq_ways // (2 * items)
    own_rows, width = rgl.shape
    shard = width // dp_ways
    length, head_cols = heads.shape
    tokens = own_rows // items
    half = tokens // 2
    unit_rows = g2.shape[0] // chips
    units_half = g1.shape[1]
    gp_rows, gp_cols = gp.shape
    block_p = gp_rows // dp_ways
    gq_cols = ranks * 3 * head_cols + LANES
    stage_rows = max(own_rows, seq_ways * half)
    any_spec = pl.BlockSpec(memory_space=pl.ANY)
    vmem_spec = pl.BlockSpec(memory_space=pltpu.VMEM)
    low = lambda *shape: pltpu.VMEM(shape, bf16)

    def share(rows, cols):
        return [
            low(chips - 1, rows, cols),
            low(rows, cols),
            low(seq_ways - 1, rows // seq_ways, cols),
            low(rows, cols),
        ]

    remotes = 96
    return pl.pallas_call(
        functools.partial(backward_kernel, items),
        in_specs=[any_spec] * 10 + [vmem_spec],
        out_specs=[any_spec] * 3 + [vmem_spec] * 3,
        out_shape=[
            jax.ShapeDtypeStruct((ranks * own_rows, width), bf16),
            jax.ShapeDtypeStruct((unit_rows, width), bf16),
            jax.ShapeDtypeStruct((block_p, gp_cols), bf16),
            jax.ShapeDtypeStruct((shard, 2 * units_half), bf16),
            jax.ShapeDtypeStruct((shard, 3 * width), bf16),
            jax.ShapeDtypeStruct((16, LANES), f32),
        ],
        scratch_shapes=[
            low(stage_rows, width),
            low(width, width),
            low(length, 3 * head_cols),
            low(length, head_cols),
            low(length, width),
            low(width, 3 * head_cols),
            pltpu.VMEM(small.shape, f32),
            low(stage_rows, width),
            low(length, head_cols),
            low(length, width),
            low(length, 3 * head_cols),
            pltpu.VMEM((seq_ways * half, width), f32),
            low(seq_ways * half, width),
            pltpu.VMEM((8, 2 * width), f32),
            low(LANES, length),
            pltpu.VMEM((length, LANES), f32),
            pltpu.VMEM((length, LANES), f32),
            *share(unit_rows, width),
            *share(2 * shard, units_half),
            low(gp_rows // 2, gp_cols),
            low(gp_rows // 2, gp_cols),
            *share(block_p, gp_cols),
            low(width, gq_cols),
            *share(2 * shard, gq_cols),
            low(shard, units_half),
            low(shard, gq_cols),
            low(16, LANES),
            pltpu.SemaphoreType.DMA((remotes,)),
            pltpu.SemaphoreType.DMA((remotes,)),
            pltpu.SemaphoreType.DMA((32,)),
            pltpu.SemaphoreType.DMA((2 * items * ranks,)),
            pltpu.SemaphoreType.DMA((seq_ways,)),
            pltpu.SemaphoreType.DMA((seq_ways,)),
            pltpu.SemaphoreType.DMA,
        ],
        compiler_params=pltpu.CompilerParams(
            collective_id=1, has_side_effects=True, vmem_limit_bytes=67043328
        ),
        name="backward",
    )(rgl, wp, g2, g1, gp, prj, heads, img, wq, small, lse)


def body(
    images,
    qkv_weight,
    qv_bias,
    proj_weight,
    proj_bias,
    ln1_gain,
    ln1_bias,
    ln2_gain,
    ln2_bias,
    fc1_weight,
    fc1_bias,
    fc2_weight,
    fc2_bias,
    cotangent,
):
    items, tokens, width = images.shape
    own_rows = items * tokens
    seq_ways, dp_ways = lax.axis_size("seq"), lax.axis_size("dp")
    chips = dp_ways // 2
    shard_rows = width // dp_ways
    column_items = 2 * items
    ranks = seq_ways // column_items
    groups = 2 * ranks
    head_cols = width // groups
    length = seq_ways * tokens
    half = tokens // 2
    dp_index, seq_index = lax.axis_index("dp"), lax.axis_index("seq")
    core, chip = dp_index % 2, dp_index // 2
    first_core = core == 0
    rank = seq_index % ranks
    group = rank * 2 + core
    same_core = [[2 * q + c for q in range(chips)] for c in range(2)]

    def swap(array):
        return lax.ppermute(array, "dp", [(i, i ^ 1) for i in range(dp_ways)])

    def by_core(own, other, axis):
        return jnp.where(
            first_core, jnp.stack([own, other], axis), jnp.stack([other, own], axis)
        )

    def pick(array, index, axis):
        return lax.dynamic_index_in_dim(array, index, axis, keepdims=False)

    def hop(array, bits):
        return lax.ppermute(array, "dp", [(i, i ^ (2 * bits)) for i in range(dp_ways)])

    def gather_chips(block):
        if chips != 4:
            return lax.all_gather(block, "dp", axis=0, axis_index_groups=same_core)
        gathered = jnp.zeros((4,) + block.shape, block.dtype)
        gathered = lax.dynamic_update_index_in_dim(gathered, block, chip, 0)
        for bits in (1, 2, 3):
            gathered = lax.dynamic_update_index_in_dim(gathered, hop(block, bits), chip ^ bits, 0)
        return gathered

    def scatter_chips(blocks):
        if chips != 4:
            return lax.psum_scatter(
                blocks, "dp", scatter_dimension=0, tiled=False, axis_index_groups=same_core
            )
        total = pick(blocks, chip, 0).astype(f32)
        for bits in (1, 2, 3):
            total = total + hop(pick(blocks, chip ^ bits, 0), bits).astype(f32)
        return total.astype(bf16)

    small_names = (qv_bias, proj_bias, ln1_gain, ln1_bias, ln2_gain, ln2_bias, fc1_bias, fc2_bias)
    small = jnp.concatenate(small_names).astype(f32)
    cotangent_own = cotangent.reshape(own_rows, width)
    (
        image_low,
        qkv_full,
        proj_full,
        fc1_half,
        fc2_half,
        cotangent_all,
        small,
        projected,
        attended,
        log_total,
        attended_rows,
    ) = forward(
        items,
        images.reshape(own_rows, width),
        qkv_weight,
        proj_weight,
        fc1_weight,
        fc2_weight,
        cotangent_own,
        jnp.broadcast_to(small, (8, small.shape[0])),
    )
    small_all = small
    small = small.reshape(dp_ways, 8, -1)[:, 0]
    smalls, at = [], 0
    for array in small_names:
        smalls.append(small[:, at : at + array.shape[0]].reshape(-1))
        at += array.shape[0]
    _, bias_proj, gain_first, shift_first, gain_second, shift_second, bias_one, bias_two = smalls
    bias_one_half = pick(bias_one.reshape(chips, 2, -1), core, 1).reshape(-1)
    flat_rows = images.reshape(own_rows, width).astype(f32)
    residual_first = flat_rows + dot(attended_rows, proj_full) + bias_proj
    normed_second, inv_second = norm_stats(residual_first)
    hidden_own = (normed_second * gain_second + shift_second).astype(bf16)
    hidden_second = by_core(hidden_own, swap(hidden_own), 0).reshape(2 * own_rows, width)
    pre_act = dot(hidden_second, fc1_half) + bias_one_half
    acts = (pre_act * gelu_cdf(pre_act)).astype(bf16)

    def meet(partial):
        parts = partial.reshape(2, own_rows, width)
        return pick(parts, core, 0) + swap(pick(parts, 1 - core, 0).astype(bf16)).astype(f32)

    output = residual_first + meet(dot(acts, fc2_half)) + bias_two

    pre_grad = dot(cotangent_all, fc2_half, 1, 1) * gelu_slope(pre_act)
    pre_grad_low = pre_grad.astype(bf16)
    grad_bias_one = jnp.sum(pre_grad, axis=0)
    grad_out = cotangent_own.astype(f32)
    grad_bias_two = jnp.sum(grad_out, axis=0)
    hidden_second_grad = meet(dot(pre_grad_low, fc1_half, 1, 1))
    grad_gain_second = jnp.sum(hidden_second_grad * normed_second, axis=0)
    grad_shift_second = jnp.sum(hidden_second_grad, axis=0)
    residual_grad = grad_out + norm_backward(
        hidden_second_grad, normed_second, inv_second, gain_second
    )
    residual_grad_low = residual_grad.astype(bf16)
    grad_proj_bias = jnp.sum(residual_grad, axis=0)
    grad_fc_two = dot(acts, cotangent_all, 0, 0).astype(bf16)
    grad_fc_one = dot(hidden_second, pre_grad_low, 0, 0).astype(bf16)
    grad_proj = dot(attended_rows, residual_grad_low, 0, 0).astype(bf16)

    def shares(vector):
        return vector.reshape(dp_ways, -1)

    one_parts = grad_bias_one.reshape(chips, 1, -1)
    one_all = jnp.where(
        jnp.arange(2)[None, :, None] == core, jnp.broadcast_to(one_parts, (chips, 2, one_parts.shape[2])), 0.0
    )
    block_rows = -(-shard_rows // (16 * seq_ways)) * 16 * seq_ways

    def by_owner(array):
        array = array.reshape((chips, 2) + array.shape[1:])
        return jnp.moveaxis(array, 1, 0)

    extra = jnp.concatenate(
        [
            shares(grad_proj_bias),
            shares(grad_gain_second),
            shares(grad_shift_second),
            shares(grad_bias_two),
            shares(one_all),
        ],
        axis=1,
    )
    extra = extra.reshape(dp_ways, -1, LANES).astype(bf16)
    extra_rows = extra.shape[1]
    extra = jnp.pad(extra, ((0, 0), (0, shard_rows - extra_rows), (0, 0)))
    blocks = jnp.concatenate([grad_proj.reshape(dp_ways, shard_rows, width), extra], axis=2)
    blocks = jnp.pad(blocks, ((0, 0), (0, block_rows - shard_rows), (0, 0)))
    blocks = by_owner(blocks).reshape(dp_ways * block_rows, width + LANES)

    home, share_two, share_proj, out_one, out_qkv, first_sums = backward(
        items,
        residual_grad_low,
        proj_full,
        grad_fc_two,
        grad_fc_one,
        blocks,
        projected,
        attended,
        image_low,
        qkv_full,
        small_all,
        log_total,
    )
    home = home.reshape(ranks, own_rows, width).astype(f32)
    hidden_first_grad = jnp.sum(home, axis=0) if ranks > 1 else home[0]
    normed_first, inv_first = norm_stats(flat_rows)
    image_grad = residual_grad + norm_backward(
        hidden_first_grad, normed_first, inv_first, gain_first
    )
    per_chip = 2 * shard_rows
    first_sums = first_sums.reshape(-1)
    out_gain_first = pick(first_sums[:per_chip].reshape(2, -1), core, 0)
    out_shift_first = pick(first_sums[per_chip : 2 * per_chip].reshape(2, -1), core, 0)
    out_qv = pick(first_sums[2 * per_chip : 4 * per_chip].reshape(2, -1), core, 0)
    last = share_proj[:extra_rows, width:].reshape(-1).astype(f32)
    out_smalls, at = [], 0
    for size in (shard_rows, shard_rows, shard_rows, shard_rows, 4 * shard_rows):
        out_smalls.append(last[at : at + size])
        at += size
    return (
        output.reshape(images.shape),
        image_grad.reshape(images.shape),
        out_qkv.astype(f32),
        out_qv,
        share_proj[:shard_rows, :width].astype(f32),
        out_smalls[0],
        out_gain_first,
        out_shift_first,
        out_smalls[1],
        out_smalls[2],
        out_one.astype(f32),
        out_smalls[4],
        share_two.astype(f32),
        out_smalls[3],
    )


def solution(mesh):
    rows, cols, flat = P("dp", "seq", None), P("dp", None), P("dp")
    in_specs = (rows, cols, flat, cols, flat, flat, flat, flat, flat, cols, flat, cols, flat, rows)
    out_specs = (rows, rows, cols, flat, cols, flat, flat, flat, flat, flat, cols, flat, cols, flat)
    return jax.shard_map(body, mesh=mesh, in_specs=in_specs, out_specs=out_specs, check_vma=False)
```

```python
import functools

import jax
import jax.numpy as jnp
from jax import lax
from jax.experimental import pallas as pl
from jax.experimental.pallas import tpu as pltpu
from jax.sharding import PartitionSpec as P

HEAD_DIM = 64
LANES = 128
f32 = jnp.float32
bf16 = jnp.bfloat16

epsilon = 1e-06


def norm_stats(matrix):
    mean_val = jnp.mean(matrix, axis=-1, keepdims=True)
    centred = matrix - mean_val
    inv_std = lax.rsqrt(jnp.mean(centred * centred, axis=-1, keepdims=True) + epsilon)
    return (centred * inv_std, inv_std)


def norm_backward(grad_in, normed, inv_std, gain):
    scaled = grad_in * gain
    return inv_std * (
        scaled
        - jnp.mean(scaled, axis=-1, keepdims=True)
        - normed * jnp.mean(scaled * normed, axis=-1, keepdims=True)
    )


def gelu_cdf(pre_act):
    return 0.5 * (1.0 + lax.erf(pre_act * 0.7071067811865476))


def gelu_slope(pre_act):
    return gelu_cdf(pre_act) + pre_act * jnp.exp(-0.5 * pre_act * pre_act) * 0.3989422804014327


def dot(left, right, left_dim=1, right_dim=0):
    return lax.dot_general(
        left, right, (((left_dim,), (right_dim,)), ((), ())), preferred_element_type=f32
    )


def transpose_low(matrix):
    return matrix.astype(f32).T.astype(bf16)


def pair_masks():
    lane = lax.broadcasted_iota(jnp.int32, (1, LANES), 1)
    return (lane < HEAD_DIM, lane >= HEAD_DIM)


def attend_kernel(q_ref, k_ref, v_ref, out_ref, lse_ref, v_flip):
    @pl.when(pl.program_id(1) == 0)
    def _():
        v_flip[...] = transpose_low(v_ref[...])

    query = q_ref[...] * jnp.asarray(HEAD_DIM**-0.5, bf16)
    key = k_ref[...]
    pieces = []
    for head, mask in enumerate(pair_masks()):
        scores = dot(key, jnp.where(mask, query, jnp.zeros_like(query)), 1, 1)
        peak = jnp.max(scores, axis=0, keepdims=True)
        lifted = jnp.exp(scores - peak)
        total = jnp.sum(lifted, axis=0, keepdims=True)
        probs = (lifted * (1.0 / total)).astype(bf16)
        rows = slice(head * HEAD_DIM, (head + 1) * HEAD_DIM)
        pieces.append(dot(v_flip[rows, :], probs))
        lse_ref[0, head : head + 1, :] = peak + jnp.log(total)
    out_ref[...] = jnp.concatenate(pieces, axis=0).T.astype(bf16)


def attend_back_kernel(
    q_ref, k_ref, v_ref, out_ref, grad_ref, lse_ref, all_ref, sums_ref, k_flip, dk_sum, dv_sum
):
    pair, block = pl.program_id(0), pl.program_id(1)
    pairs, blocks = pl.num_programs(0), pl.num_programs(1)
    block_rows = q_ref.shape[0]

    @pl.when(block == 0)
    def _():
        k_flip[...] = transpose_low(k_ref[...])
        dk_sum[...] = jnp.zeros_like(dk_sum)
        dv_sum[...] = jnp.zeros_like(dv_sum)
        sums_ref[...] = jnp.zeros_like(sums_ref)

    query = q_ref[...] * jnp.asarray(HEAD_DIM**-0.5, bf16)
    key = k_ref[...]
    value = v_ref[...]
    grad = grad_ref[...]
    mixed = (grad.astype(f32) * out_ref[...].astype(f32)).T
    pieces = []
    for head, mask in enumerate(pair_masks()):
        rows = slice(head * HEAD_DIM, (head + 1) * HEAD_DIM)
        query_one = jnp.where(mask, query, jnp.zeros_like(query))
        grad_one = jnp.where(mask, grad, jnp.zeros_like(grad))
        probs = jnp.exp(dot(key, query_one, 1, 1) - lse_ref[0, head : head + 1, :])
        prob_grad = dot(value, grad_one, 1, 1)
        delta = jnp.sum(mixed[rows], axis=0, keepdims=True)
        score_grad = (probs * (prob_grad - delta) * HEAD_DIM**-0.5).astype(bf16)
        dv_sum[...] += dot(probs.astype(bf16), grad_one)
        dk_sum[...] += dot(score_grad, query_one)
        pieces.append(dot(k_flip[rows, :], score_grad))
    query_grad = jnp.concatenate(pieces, axis=0).T
    row_at = pl.multiple_of(block * block_rows, block_rows)
    lanes = pl.ds(pl.multiple_of(pair * LANES, LANES), LANES)
    all_ref[pl.ds(row_at, block_rows), lanes] = query_grad.astype(bf16)
    sums_ref[0, 0:1, :] += jnp.sum(query_grad, axis=0, keepdims=True)

    @pl.when(block == blocks - 1)
    def _():
        key_lanes = pl.ds(pl.multiple_of((pairs + pair) * LANES, LANES), LANES)
        value_lanes = pl.ds(pl.multiple_of((2 * pairs + pair) * LANES, LANES), LANES)
        all_ref[:, key_lanes] = (dk_sum[...] * HEAD_DIM**0.5).astype(bf16)
        all_ref[:, value_lanes] = dv_sum[...].astype(bf16)
        sums_ref[0, 1:2, :] = jnp.sum(dv_sum[...], axis=0, keepdims=True)


def block_size(length):
    return next(
        size
        for size in (384, 256, 128, length)
        if length % size == 0 and (size * length <= 384 * 1152 or size <= 128 or size == length)
    )


def attend(projected):
    length, head_cols = projected.shape[0], projected.shape[1] // 3
    pairs = head_cols // LANES
    rows = block_size(length)
    query_spec = pl.BlockSpec((rows, LANES), lambda h, b: (b, h))
    return pl.pallas_call(
        attend_kernel,
        grid=(pairs, length // rows),
        in_specs=[
            query_spec,
            pl.BlockSpec((length, LANES), lambda h, b: (0, pairs + h)),
            pl.BlockSpec((length, LANES), lambda h, b: (0, 2 * pairs + h)),
        ],
        out_specs=[query_spec, pl.BlockSpec((1, 2, rows), lambda h, b: (h, 0, b))],
        out_shape=[
            jax.ShapeDtypeStruct((length, head_cols), bf16),
            jax.ShapeDtypeStruct((pairs, 2, length), f32),
        ],
        scratch_shapes=[pltpu.VMEM((LANES, length), bf16)],
        compiler_params=pltpu.CompilerParams(vmem_limit_bytes=58 * 2**20),
        cost_estimate=pl.CostEstimate(
            flops=16 * pairs * length * length * LANES,
            bytes_accessed=8 * length * head_cols,
            transcendentals=2 * pairs * length * length,
        ),
        name="attend",
    )(projected, projected, projected)


def attend_back(projected, attended, log_total, grad):
    length, head_cols = attended.shape
    pairs = head_cols // LANES
    rows = block_size(length)
    query_spec = pl.BlockSpec((rows, LANES), lambda h, b: (b, h))
    return pl.pallas_call(
        attend_back_kernel,
        grid=(pairs, length // rows),
        in_specs=[
            query_spec,
            pl.BlockSpec((length, LANES), lambda h, b: (0, pairs + h)),
            pl.BlockSpec((length, LANES), lambda h, b: (0, 2 * pairs + h)),
            query_spec,
            query_spec,
            pl.BlockSpec((1, 2, rows), lambda h, b: (h, 0, b)),
        ],
        out_specs=[
            pl.BlockSpec((length, 3 * head_cols), lambda h, b: (0, 0)),
            pl.BlockSpec((1, 2, LANES), lambda h, b: (h, 0, 0)),
        ],
        out_shape=[
            jax.ShapeDtypeStruct((length, 3 * head_cols), bf16),
            jax.ShapeDtypeStruct((pairs, 2, LANES), f32),
        ],
        scratch_shapes=[
            pltpu.VMEM((LANES, length), bf16),
            pltpu.VMEM((length, LANES), f32),
            pltpu.VMEM((length, LANES), f32),
        ],
        compiler_params=pltpu.CompilerParams(vmem_limit_bytes=58 * 2**20),
        cost_estimate=pl.CostEstimate(
            flops=40 * pairs * length * length * LANES,
            bytes_accessed=16 * length * head_cols,
            transcendentals=2 * pairs * length * length,
        ),
        name="attend_back",
    )(projected, projected, projected, attended, grad, log_total)


class Copies:
    def __init__(self, send_sems, recv_sems, local_sems):
        self.send_sems, self.recv_sems, self.local_sems = send_sems, recv_sems, local_sems
        self.sent, self.locals, self.local_count = [], [], 0

    def remote(self, src, dst, **device):
        copy = self.prepare(src, dst, **device)
        copy.start()
        return copy

    def prepare(self, src, dst, **device):
        at = len(self.sent)
        copy = pltpu.make_async_remote_copy(
            src_ref=src,
            dst_ref=dst,
            send_sem=self.send_sems.at[at],
            recv_sem=self.recv_sems.at[at],
            device_id=device,
            device_id_type=pl.DeviceIdType.MESH,
        )
        self.sent.append(copy)
        return copy

    def local(self, src, dst):
        copy = self.prepare_local(src, dst)
        copy.start()
        self.locals.append(copy)
        return copy

    def prepare_local(self, src, dst):
        copy = pltpu.make_async_copy(src, dst, self.local_sems.at[self.local_count])
        self.local_count += 1
        return copy

    def wait_local(self, copy):
        copy.wait()
        self.locals = [kept for kept in self.locals if kept is not copy]

    def finish(self):
        for copy in self.sent:
            copy.wait_send()
        for copy in self.locals:
            copy.wait()


class Place:
    def __init__(self, items):
        self.dp_ways, self.seq_ways = lax.axis_size("dp"), lax.axis_size("seq")
        self.chips = self.dp_ways // 2
        self.ranks = self.seq_ways // (2 * items)
        self.dp, self.seq = lax.axis_index("dp"), lax.axis_index("seq")
        self.core, self.chip = lax.rem(self.dp, 2), lax.div(self.dp, 2)
        self.rank = lax.rem(self.seq, self.ranks)
        self.item = lax.div(self.seq, self.ranks)

    def partner(self, offset):
        if self.chips == 4:
            x, y = lax.rem(self.chip, 2), lax.div(self.chip, 2)
            x = 1 - x if offset % 2 else x
            y = 1 - y if offset >= 2 else y
            return y * 2 + x
        return lax.rem(self.chip + offset, self.chips)

    def source(self, offset):
        if self.chips == 4:
            return self.partner(offset)
        return lax.rem(self.chip + self.chips - offset, self.chips)

    def meet(self):
        barrier = pltpu.get_barrier_semaphore()
        for step in range(1, self.dp_ways):
            pl.semaphore_signal(
                barrier,
                inc=1,
                device_id={"dp": lax.rem(self.dp + step, self.dp_ways)},
                device_id_type=pl.DeviceIdType.MESH,
            )
        for step in range(1, self.seq_ways):
            for core in range(2):
                pl.semaphore_signal(
                    barrier,
                    inc=1,
                    device_id={
                        "dp": self.chip * 2 + core,
                        "seq": lax.rem(self.seq + step, self.seq_ways),
                    },
                    device_id_type=pl.DeviceIdType.MESH,
                )
        pl.semaphore_wait(barrier, self.dp_ways - 1 + 2 * (self.seq_ways - 1))


def rows_at(start, size):
    return pl.ds(pl.multiple_of(start, 16), size)


def lanes_at(start, size):
    return pl.ds(pl.multiple_of(start, LANES), size)


def attend_rows(prj, out, lse, v_flip, pair, block, rows):
    pairs = out.shape[1] // LANES
    query = prj[rows_at(block * rows, rows), lanes_at(pair * LANES, LANES)]
    query = query * jnp.asarray(HEAD_DIM**-0.5, bf16)
    key = prj[:, lanes_at((pairs + pair) * LANES, LANES)]
    pieces = []
    for head, mask in enumerate(pair_masks()):
        scores = dot(key, jnp.where(mask, query, jnp.zeros_like(query)), 1, 1)
        peak = jnp.max(scores, axis=0, keepdims=True)
        lifted = jnp.exp(scores - peak)
        total = jnp.sum(lifted, axis=0, keepdims=True)
        probs = (lifted * (1.0 / total)).astype(bf16)
        pieces.append(dot(v_flip[head * HEAD_DIM : (head + 1) * HEAD_DIM, :], probs))
        lse[pair, head : head + 1, lanes_at(block * rows, rows)] = peak + jnp.log(total)
    out[rows_at(block * rows, rows), lanes_at(pair * LANES, LANES)] = (
        jnp.concatenate(pieces, axis=0).T.astype(bf16)
    )


def forward_kernel(
    items,
    img,
    wq,
    wp,
    w1,
    w2,
    cot,
    small,
    img_out,
    wq_out,
    wp_out,
    w1_out,
    w2_out,
    cot_out,
    small_out,
    prj_out,
    heads_out,
    lse_out,
    rows_out,
    res_out,
    hid_out,
    pre_out,
    acts_out,
    img_v,
    wq_v,
    prj_v,
    heads_v,
    small_v,
    vec_v,
    v_flip,
    wp_v,
    w1_v,
    rows_v,
    own_v,
    res_v,
    hid_v,
    pre_v,
    acts_v,
    send_sems,
    recv_sems,
    local_sems,
    token_send,
    token_recv,
    back_send,
    back_recv,
):
    at = Place(items)
    chips, ranks, seq_ways, dp_ways = at.chips, at.ranks, at.seq_ways, at.dp_ways
    tokens = img.shape[0] // items
    half = tokens // 2
    shard, width = wp.shape
    head_cols = heads_v.shape[1]
    unit_rows = w2.shape[0]
    length = img_v.shape[0]
    pairs = head_cols // LANES
    relay = chips == 4
    offsets = (1, 2) if relay else tuple(range(1, chips))
    copies = Copies(send_sems, recv_sems, local_sems)
    at.meet()
    me = rows_at(at.dp * shard, shard)

    token_jobs = []
    for item in range(items):
        for k in range(ranks):
            for h in range(2):
                to_seq = (at.core * items + item) * ranks + k
                mine = (to_seq == at.seq) & (at.core == h)
                src = img.at[pl.ds(item * tokens + h * half, half), :]
                dst = img_v.at[rows_at(at.seq * tokens + h * half, half), :]
                sem = token_send.at[len(token_jobs)]
                far = pltpu.make_async_remote_copy(
                    src_ref=src,
                    dst_ref=dst,
                    send_sem=sem,
                    recv_sem=token_recv.at[at.seq],
                    device_id={"dp": at.chip * 2 + h, "seq": to_seq},
                    device_id_type=pl.DeviceIdType.MESH,
                )
                near = pltpu.make_async_copy(src, dst, token_recv.at[at.seq])
                pl.when(mine)(near.start)
                pl.when(jnp.logical_not(mine))(far.start)
                token_jobs.append((mine, far))

    other = at.chip * 2 + 1 - at.core
    small_copies = []
    small_rows = rows_at(at.dp * 16, 16)
    small_own = copies.local(small, small_v.at[small_rows, :])
    for step in range(1, dp_ways):
        small_copies.append(
            copies.remote(small, small_v.at[small_rows, :], dp=lax.rem(at.dp + step, dp_ways))
        )

    def qkv_pieces(core):
        group = at.rank * 2 + core
        return [
            (
                wq.at[:, lanes_at(part * width + group * head_cols, head_cols)],
                wq_v.at[me, pl.ds(part * head_cols, head_cols)],
            )
            for part in range(3)
        ]

    def fc1_pieces(core):
        return [
            (
                w1.at[:, lanes_at((2 * q + core) * unit_rows, unit_rows)],
                w1_v.at[me, pl.ds(q * unit_rows, unit_rows)],
            )
            for q in range(chips)
        ]

    def start_columns(pieces):
        arrivals = {0: [], "local": [copies.local(src, dst) for src, dst in pieces(at.core)]}
        for src, dst in pieces(1 - at.core):
            arrivals[0].append(copies.remote(src, dst, dp=other))
        for offset in offsets:
            for core in (at.core, 1 - at.core):
                for src, dst in pieces(core):
                    copy = copies.remote(src, dst, dp=at.partner(offset) * 2 + core)
                    arrivals.setdefault(offset, []).append(copy)
        return arrivals

    def pass_on(arrivals, block_of, first, second):
        for copy in arrivals[1]:
            copy.wait_recv()
        last = []
        if relay:
            ref = block_of(at.partner(1), *first)
            last.append(copies.remote(ref, ref, dp=at.partner(2) * 2 + at.core))
        for copy in arrivals[2]:
            copy.wait_recv()
        if relay:
            ref = block_of(at.partner(2), *second)
            last.append(copies.remote(ref, ref, dp=at.partner(1) * 2 + at.core))
        for offset in range(3, chips):
            if not relay:
                for copy in arrivals[offset]:
                    copy.wait_recv()
        return last

    def settle(arrivals, last):
        for copy in last:
            copy.wait_recv()
        for copy in arrivals[0]:
            copy.wait_recv()

    def shard_halves(ref):
        return lambda chip, start, size: ref.at[rows_at(chip * 2 * shard + start, size), :]

    qkv_arrivals = start_columns(qkv_pieces)

    wp_near = [copies.remote(wp, wp_v.at[me, :], dp=other)]
    wp_own = copies.local(wp, wp_v.at[me, :])
    own_copy = copies.local(img, own_v)
    wp_far = {
        o: [copies.remote(wp, wp_v.at[me, :], dp=at.partner(o) * 2 + at.core)] for o in offsets
    }
    cot_rows = rows_at(at.core * cot.shape[0], cot.shape[0])
    cot_near = copies.remote(cot, cot_out.at[cot_rows, :], dp=other)
    copies.local(cot, cot_out.at[cot_rows, :])

    for s in range(seq_ways):
        pltpu.make_async_copy(
            img.at[pl.ds(0, half), :], img_v.at[pl.ds(s * tokens, half), :], token_recv.at[s]
        ).wait()
    for mine, far in token_jobs:
        pl.when(jnp.logical_not(mine))(far.wait_send)
    token_near = []
    for s in range(seq_ways):
        ref = img_v.at[rows_at(s * tokens + at.core * half, half), :]
        token_near.append(copies.remote(ref, ref, dp=other))
    qkv_last = pass_on(qkv_arrivals, shard_halves(wq_v), (0, shard), (shard, shard))
    fc1_arrivals = start_columns(fc1_pieces)
    w2_to = lambda chip: w2_out.at[rows_at(chip * unit_rows, unit_rows), :]
    copies.local(w2, w2_to(at.chip))
    fc2_arrivals = {0: []}
    for offset in offsets:
        fc2_arrivals[offset] = [
            copies.remote(w2, w2_to(at.chip), dp=at.partner(offset) * 2 + at.core)
        ]

    for copy in small_copies:
        copy.wait_recv()
    copies.wait_local(small_own)
    for row, start, size in ((0, 0, 2), (1, 3, 1), (2, 4, 1), (4, 2, 1), (5, 5, 1), (6, 6, 1)):
        for i in range(dp_ways):
            for j in range(size):
                lane = (i * size + j) * shard
                line = 16 * i + start + j
                vec_v[row : row + 1, lane : lane + shard] = small_v[line : line + 1, :shard]
    for q in range(chips):
        for j in range(4):
            lane = (q * 4 + j) * shard
            line = pl.ds((2 * q + at.core) * 16 + 7 + j, 1)
            vec_v[3:4, lane : lane + shard] = small_v[line, :shard]
    for copy in token_near:
        copy.wait_recv()
    settle(qkv_arrivals, qkv_last)
    for copy in qkv_arrivals["local"]:
        copies.wait_local(copy)

    group = at.rank * 2 + at.core
    gain = vec_v[1:2, :width]
    shift = vec_v[2:3, :width]

    def project(step, carry):
        rows = rows_at(step * tokens, tokens)
        normed, _ = norm_stats(img_v[rows, :].astype(f32))
        hidden = (normed * gain + shift).astype(bf16)
        for part in range(3):
            cols = slice(part * head_cols, (part + 1) * head_cols)
            block = dot(hidden, wq_v[:, cols])
            if part != 1:
                lanes = lanes_at((part // 2) * width + group * head_cols, head_cols)
                block = block + vec_v[0:1, lanes]
            prj_v[rows, cols] = block.astype(bf16)
        return carry

    lax.fori_loop(0, seq_ways, project, 0)
    copies.local(img_v, img_out)
    copies.local(wq_v, wq_out)
    copies.local(prj_v, prj_out)
    copies.local(small_v, small_out)

    rows = block_size(length)
    home_core = lax.div(at.item, items)
    home_item = lax.rem(at.item, items)

    def back_copies(pair):
        jobs = []
        for s in range(seq_ways):
            mine = (at.seq == s) & (at.core == home_core)
            src = heads_v.at[pl.ds(s * tokens, tokens), lanes_at(pair * LANES, LANES)]
            dst = rows_v.at[
                rows_at(home_item * tokens, tokens),
                lanes_at(group * head_cols + pair * LANES, LANES),
            ]
            far = pltpu.make_async_remote_copy(
                src_ref=src,
                dst_ref=dst,
                send_sem=back_send.at[pair, s],
                recv_sem=back_recv,
                device_id={"dp": at.chip * 2 + home_core, "seq": s},
                device_id_type=pl.DeviceIdType.MESH,
            )
            near = pltpu.make_async_copy(src, dst, back_recv)
            jobs.append((mine, far, near))
        return jobs

    def one_pair(pair, carry):
        v_flip[...] = transpose_low(prj_v[:, lanes_at((2 * pairs + pair) * LANES, LANES)])

        def one_block(block, inner):
            attend_rows(prj_v, heads_v, lse_out, v_flip, pair, block, rows)
            return inner

        lax.fori_loop(0, length // rows, one_block, 0)
        for mine, far, near in back_copies(pair):
            pl.when(mine)(near.start)
            pl.when(jnp.logical_not(mine))(far.start)
        return carry

    lax.fori_loop(0, pairs, one_pair, 0)
    copies.local(heads_v, heads_out)
    wp_last = pass_on(
        wp_far,
        lambda chip, start, size: wp_v.at[
            rows_at((chip * 2 + at.core) * shard + start, size), :
        ],
        (0, shard // 2),
        (shard // 2, shard // 2),
    )
    fc1_last = pass_on(fc1_arrivals, shard_halves(w1_v), (0, shard), (shard, shard))
    for copy in wp_last:
        copy.wait_recv()
    for offset in range(1, chips):
        ref = wp_v.at[rows_at((at.source(offset) * 2 + at.core) * shard, shard), :]
        wp_near.append(copies.remote(ref, ref, dp=other))
    fc2_last = pass_on(
        fc2_arrivals,
        lambda chip, start, size: w2_out.at[rows_at(chip * unit_rows + start, size), :],
        (0, unit_rows // 2),
        (unit_rows // 2, unit_rows // 2),
    )
    for copy in wp_near:
        copy.wait_recv()
    copies.wait_local(wp_own)
    copies.local(wp_v, wp_out)
    copies.wait_local(own_copy)
    pltpu.make_async_copy(rows_v, rows_v, back_recv).wait()
    copies.local(rows_v, rows_out)
    own_rows = rows_v.shape[0]

    def rejoin(item, carry):
        rows = rows_at(item * tokens, tokens)
        residual = own_v[rows, :].astype(f32) + dot(rows_v[rows, :], wp_v[...]) + vec_v[4:5, :width]
        res_v[rows, :] = residual
        normed, _ = norm_stats(residual)
        hidden = normed * vec_v[5:6, :width] + vec_v[6:7, :width]
        hid_v[rows_at(at.core * own_rows + item * tokens, tokens), :] = hidden.astype(bf16)
        return carry

    lax.fori_loop(0, items, rejoin, 0)
    hid_own = hid_v.at[rows_at(at.core * own_rows, own_rows), :]
    hid_near = copies.remote(hid_own, hid_own, dp=other)
    copies.local(res_v, res_out)
    settle(fc1_arrivals, fc1_last)
    for copy in fc1_arrivals["local"]:
        copies.wait_local(copy)
    copies.local(w1_v, w1_out)
    hid_near.wait_recv()
    copies.local(hid_v, hid_out)

    def widen(step, carry):
        rows = rows_at(step * tokens, tokens)
        pre_act = dot(hid_v[rows, :], w1_v[...]) + vec_v[3:4, : w1_v.shape[1]]
        pre_v[rows, :] = pre_act
        acts_v[rows, :] = (pre_act * gelu_cdf(pre_act)).astype(bf16)
        return carry

    lax.fori_loop(0, 2 * items, widen, 0)
    copies.local(pre_v, pre_out)
    copies.local(acts_v, acts_out)
    settle(fc2_arrivals, fc2_last)
    cot_near.wait_recv()

    def drain(pair, carry):
        for mine, far, _ in back_copies(pair):
            pl.when(jnp.logical_not(mine))(far.wait_send)
        return carry

    lax.fori_loop(0, pairs, drain, 0)
    copies.finish()


def forward(items, img, wq, wp, w1, w2, cot, small):
    dp_ways, seq_ways = lax.axis_size("dp"), lax.axis_size("seq")
    ranks = seq_ways // (2 * items)
    shard, width = wp.shape
    head_cols = width // (2 * ranks)
    tokens = img.shape[0] // items
    length = seq_ways * tokens
    half_units = w1.shape[1] // 2
    pairs = head_cols // LANES
    any_spec = pl.BlockSpec(memory_space=pl.ANY)
    out_shape = [
        jax.ShapeDtypeStruct((length, width), bf16),
        jax.ShapeDtypeStruct((width, 3 * head_cols), bf16),
        jax.ShapeDtypeStruct((width, width), bf16),
        jax.ShapeDtypeStruct((width, half_units), bf16),
        jax.ShapeDtypeStruct((half_units, width), bf16),
        jax.ShapeDtypeStruct((2 * cot.shape[0], width), bf16),
        jax.ShapeDtypeStruct((16 * dp_ways, small.shape[1]), f32),
        jax.ShapeDtypeStruct((length, 3 * head_cols), bf16),
        jax.ShapeDtypeStruct((length, head_cols), bf16),
        jax.ShapeDtypeStruct((pairs, 2, length), f32),
        jax.ShapeDtypeStruct(img.shape, bf16),
        jax.ShapeDtypeStruct(img.shape, f32),
        jax.ShapeDtypeStruct((2 * img.shape[0], width), bf16),
        jax.ShapeDtypeStruct((2 * img.shape[0], half_units), f32),
        jax.ShapeDtypeStruct((2 * img.shape[0], half_units), bf16),
    ]
    out_specs = [any_spec] * len(out_shape)
    out_specs[9] = pl.BlockSpec(memory_space=pltpu.VMEM)
    remotes = 160
    return pl.pallas_call(
        functools.partial(forward_kernel, items),
        in_specs=[any_spec] * 7,
        out_specs=out_specs,
        out_shape=out_shape,
        scratch_shapes=[
            pltpu.VMEM((length, width), bf16),
            pltpu.VMEM((width, 3 * head_cols), bf16),
            pltpu.VMEM((length, 3 * head_cols), bf16),
            pltpu.VMEM((length, head_cols), bf16),
            pltpu.VMEM((16 * dp_ways, small.shape[1]), f32),
            pltpu.VMEM((8, 2 * width), f32),
            pltpu.VMEM((LANES, length), bf16),
            pltpu.VMEM((width, width), bf16),
            pltpu.VMEM((width, half_units), bf16),
            pltpu.VMEM(img.shape, bf16),
            pltpu.VMEM(img.shape, bf16),
            pltpu.VMEM(img.shape, f32),
            pltpu.VMEM((2 * img.shape[0], width), bf16),
            pltpu.VMEM((2 * img.shape[0], half_units), f32),
            pltpu.VMEM((2 * img.shape[0], half_units), bf16),
            pltpu.SemaphoreType.DMA((remotes,)),
            pltpu.SemaphoreType.DMA((remotes,)),
            pltpu.SemaphoreType.DMA((40,)),
            pltpu.SemaphoreType.DMA((2 * items * ranks,)),
            pltpu.SemaphoreType.DMA((seq_ways,)),
            pltpu.SemaphoreType.DMA((pairs, seq_ways)),
            pltpu.SemaphoreType.DMA,
        ],
        compiler_params=pltpu.CompilerParams(
            collective_id=0, has_side_effects=True, vmem_limit_bytes=67043328
        ),
        name="forward",
    )(img, wq, wp, w1, w2, cot, small)


class Share:
    def __init__(self, at, copies, block_of, slots, total, line, final):
        self.at = at
        self.slots, self.total, self.line, self.final = slots, total, line, final
        rows = total.shape[0]
        mid = rows // 2
        self.mid = mid
        self.relays = at.chips == 4
        low, high = pl.ds(0, mid), pl.ds(mid, mid)

        def to_chip(src, dst, offset):
            return copies.prepare(src, dst, dp=at.partner(offset) * 2 + at.core)

        if self.relays:
            mine, x, y, far = (block_of(at.partner(offset)) for offset in (0, 1, 2, 3))
            self.first = [
                to_chip(x.at[low, :], slots.at[0, low, :], 1),
                to_chip(far.at[low, :], slots.at[0, high, :], 1),
                to_chip(y.at[high, :], slots.at[1, low, :], 2),
                to_chip(far.at[high, :], slots.at[1, high, :], 2),
            ]
            self.loads = [
                copies.prepare_local(mine, total),
                copies.prepare_local(y.at[low, :], slots.at[2, low, :]),
                copies.prepare_local(x.at[high, :], slots.at[2, high, :]),
            ]
            self.second = [
                to_chip(slots.at[2, low, :], slots.at[3, low, :], 2),
                to_chip(slots.at[2, high, :], slots.at[3, high, :], 1),
            ]
        else:
            self.first = [
                to_chip(block_of(at.partner(offset)), slots.at[offset - 1], offset)
                for offset in range(1, at.chips)
            ]
            self.loads = [copies.prepare_local(block_of(at.chip), total)]
            self.second = []

        self.bits = at.seq_ways.bit_length() - 1
        self.regions, self.halving = [], []
        start, size, slot = 0, rows, 0
        for bit in range(self.bits):
            size //= 2
            side = lax.rem(lax.div(at.seq, 2**bit), 2)
            peer = at.seq + (1 - 2 * side) * 2**bit
            there = rows_at(start + (1 - side) * size, size)
            start = start + side * size
            here = rows_at(start, size)
            self.halving.append(
                copies.prepare(total.at[there, :], line.at[pl.ds(slot, size), :], seq=peer)
            )
            self.regions.append((start, size, slot, here, peer))
            slot += size
        self.doubling = [
            copies.prepare(final.at[here, :], final.at[here, :], seq=peer)
            for _, _, _, here, peer in reversed(self.regions)
        ]
        self.done = 0

    def spread(self):
        for copy in self.first + self.loads:
            copy.start()

    def add_rows(self, size, value_of, put):
        step = next(n for n in (64, 32, 16) if size % n == 0)

        def add(i, carry):
            put(i * step, step, value_of(i * step, step).astype(bf16))
            return carry

        lax.fori_loop(0, size // step, add, 0)

    def relay(self):
        if not self.relays:
            return
        for copy in self.first:
            copy.wait_recv()
        for copy in self.loads[1:]:
            copy.wait()
        slots, mid = self.slots, self.mid
        for side in (0, 1):

            def value(at, n):
                kept = slots[2, rows_at(side * mid + at, n), :].astype(f32)
                return kept + slots[side, rows_at(mid + at, n), :].astype(f32)

            def put(at, n, result):
                slots[2, rows_at(side * mid + at, n), :] = result

            self.add_rows(mid, value, put)
        for copy in self.second:
            copy.start()

    def add_chips(self):
        for copy in self.second if self.relays else self.first:
            copy.wait_recv()
        self.loads[0].wait()
        slots, mid, total = self.slots, self.mid, self.total

        def put(at, n, result):
            total[rows_at(at, n), :] = result

        if self.relays:
            for side in (0, 1):

                def value(at, n):
                    rows = rows_at(side * mid + at, n)
                    result = total[rows, :].astype(f32) + slots[side, rows_at(at, n), :].astype(f32)
                    return result + slots[3, rows, :].astype(f32)

                self.add_rows(mid, value, lambda at, n, result: put(side * mid + at, n, result))
        else:

            def value(at, n):
                result = total[rows_at(at, n), :].astype(f32)
                for slot in range(self.at.chips - 1):
                    result = result + slots[slot, rows_at(at, n), :].astype(f32)
                return result

            self.add_rows(2 * mid, value, put)
        self.halving[0].start()

    def step(self):
        if self.done == 2 * self.bits:
            return
        at = self.done
        self.done += 1
        if at < self.bits:
            self.halving[at].wait_recv()
            start, size, slot, _, _ = self.regions[at]
            last = at == self.bits - 1
            target = self.final if last else self.total

            def value(row, n):
                kept = self.total[rows_at(start + row, n), :].astype(f32)
                return kept + self.line[rows_at(slot + row, n), :].astype(f32)

            def put(row, n, result):
                target[rows_at(start + row, n), :] = result

            self.add_rows(size, value, put)
            (self.doubling[0] if last else self.halving[at + 1]).start()
            return
        at -= self.bits
        self.doubling[at].wait_recv()
        if at + 1 < self.bits:
            self.doubling[at + 1].start()

    def finish(self):
        while self.done < 2 * self.bits:
            self.step()


def backward_kernel(
    items,
    rgl,
    wp,
    g2,
    g1,
    gp,
    prj,
    heads,
    img,
    wq,
    small,
    lse,
    home_out,
    o2_out,
    op_out,
    o1_out,
    oq_out,
    ox_out,
    rgl_v,
    wp_v,
    prj_v,
    heads_v,
    img_v,
    wq_v,
    small_v,
    da_v,
    do_v,
    hid_v,
    dqkv_v,
    keep_v,
    near_v,
    vec_v,
    k_flip,
    dk_sum,
    dv_sum,
    slots2,
    total2,
    line2,
    final2,
    slots1,
    total1,
    line1,
    final1,
    pair_own,
    pair_far,
    slotsp,
    totalp,
    linep,
    finalp,
    ga_v,
    slotsa,
    totala,
    linea,
    finala,
    gb_v,
    slotsb,
    totalb,
    lineb,
    finalb,
    swap1,
    swapa,
    swapb,
    swapx,
    send_sems,
    recv_sems,
    local_sems,
    token_send,
    token_recv,
    home_send,
    home_recv,
):
    at = Place(items)
    chips, ranks, seq_ways = at.chips, at.ranks, at.seq_ways
    own_rows, width = rgl.shape
    tokens = own_rows // items
    half = tokens // 2
    shard = width // at.dp_ways
    head_cols = heads.shape[1]
    length = heads.shape[0]
    pairs = head_cols // LANES
    unit_rows = total2.shape[0]
    copies = Copies(send_sems, recv_sems, local_sems)
    at.meet()
    other = at.chip * 2 + 1 - at.core
    group = at.rank * 2 + at.core

    first_loads = [copies.local(rgl, rgl_v.at[pl.ds(0, own_rows), :]), copies.local(wp, wp_v)]
    pair_rows = pair_own.shape[0]
    pair_copy = copies.remote(gp.at[rows_at((1 - at.core) * pair_rows, pair_rows), :], pair_far, dp=other)
    pair_load = copies.local(gp.at[rows_at(at.core * pair_rows, pair_rows), :], pair_own)

    block_p = pair_rows // chips
    share2 = Share(
        at,
        copies,
        lambda chip: g2.at[rows_at(chip * unit_rows, unit_rows), :],
        slots2,
        total2,
        line2,
        final2,
    )
    share2.spread()
    share1 = Share(
        at,
        copies,
        lambda chip: g1.at[rows_at(chip * 2 * shard, 2 * shard), :],
        slots1,
        total1,
        line1,
        final1,
    )
    sharep = Share(
        at,
        copies,
        lambda chip: pair_own.at[rows_at(chip * block_p, block_p), :],
        slotsp,
        totalp,
        linep,
        finalp,
    )
    sharea = Share(
        at,
        copies,
        lambda chip: ga_v.at[rows_at(chip * 2 * shard, 2 * shard), :],
        slotsa,
        totala,
        linea,
        finala,
    )
    shareb = Share(
        at,
        copies,
        lambda chip: gb_v.at[rows_at(chip * 2 * shard, 2 * shard), :],
        slotsb,
        totalb,
        lineb,
        finalb,
    )
    hidden_loads = [copies.local(img, img_v), copies.local(small, small_v)]
    loads = [copies.local(prj, prj_v), copies.local(heads, heads_v), copies.local(wq, wq_v)]

    for copy in first_loads:
        copies.wait_local(copy)
    jobs = []
    for item in range(items):
        rows = pl.ds(item * tokens, tokens)
        da_v[rows, :] = dot(rgl_v[rows, :], wp_v[...], 1, 1).astype(bf16)
        for k in range(ranks):
            for h in range(2):
                to_seq = (at.core * items + item) * ranks + k
                mine = (to_seq == at.seq) & (at.core == h)
                src = da_v.at[rows, pl.ds((k * 2 + h) * head_cols, head_cols)]
                dst = do_v.at[rows_at(at.seq * tokens, tokens), :]
                far = pltpu.make_async_remote_copy(
                    src_ref=src,
                    dst_ref=dst,
                    send_sem=token_send.at[len(jobs)],
                    recv_sem=token_recv.at[at.seq],
                    device_id={"dp": at.chip * 2 + h, "seq": to_seq},
                    device_id_type=pl.DeviceIdType.MESH,
                )
                near = pltpu.make_async_copy(src, dst, token_recv.at[at.seq])
                pl.when(mine)(near.start)
                pl.when(jnp.logical_not(mine))(far.start)
                jobs.append((mine, far))

    pair_copy.wait_recv()
    copies.wait_local(pair_load)
    step = 64

    def add_pair(i, carry):
        rows = rows_at(i * step, step)
        pair_own[rows, :] = (pair_own[rows, :].astype(f32) + pair_far[rows, :].astype(f32)).astype(bf16)
        return carry

    lax.fori_loop(0, pair_rows // step, add_pair, 0)
    sharep.spread()

    for copy in hidden_loads:
        copies.wait_local(copy)
    for row, start in ((0, 3), (1, 4)):
        for i in range(at.dp_ways):
            line = 16 * i + start
            vec_v[row : row + 1, i * shard : (i + 1) * shard] = small_v[line : line + 1, :shard]
    gain = vec_v[0:1, :width]
    shift = vec_v[1:2, :width]

    wide = next(n for n in (384, 128, length) if length % n == 0)

    def hide(s, carry):
        normed, _ = norm_stats(img_v[rows_at(s * wide, wide), :].astype(f32))
        hid_v[:, lanes_at(s * wide, wide)] = (normed * gain + shift).T.astype(bf16)
        return carry

    lax.fori_loop(0, length // wide, hide, 0)
    for copy in loads:
        copies.wait_local(copy)
    share2.relay()
    share1.spread()
    sharep.relay()
    for s in range(seq_ways):
        pltpu.make_async_copy(
            do_v.at[pl.ds(s * tokens, tokens), :], do_v.at[pl.ds(s * tokens, tokens), :], token_recv.at[s]
        ).wait()
    for mine, far in jobs:
        pl.when(jnp.logical_not(mine))(far.wait_send)

    rows_q = block_size(length)
    vec_v[2:4, :] = jnp.zeros((2, vec_v.shape[1]), f32)
    vec_v[4:5, :] = jnp.zeros((1, vec_v.shape[1]), f32)

    def one_pair(pair, carry):
        q_lanes = lanes_at(pair * LANES, LANES)
        k_lanes = lanes_at((pairs + pair) * LANES, LANES)
        v_lanes = lanes_at((2 * pairs + pair) * LANES, LANES)
        k_flip[...] = transpose_low(prj_v[:, k_lanes])
        dk_sum[...] = jnp.zeros_like(dk_sum)
        dv_sum[...] = jnp.zeros_like(dv_sum)

        def one_block(block, sums):
            rows = rows_at(block * rows_q, rows_q)
            query = prj_v[rows, q_lanes] * jnp.asarray(HEAD_DIM**-0.5, bf16)
            key = prj_v[:, k_lanes]
            value = prj_v[:, v_lanes]
            grad = do_v[rows, q_lanes]
            mixed = (grad.astype(f32) * heads_v[rows, q_lanes].astype(f32)).T
            pieces = []
            for head, mask in enumerate(pair_masks()):
                span = slice(head * HEAD_DIM, (head + 1) * HEAD_DIM)
                query_one = jnp.where(mask, query, jnp.zeros_like(query))
                grad_one = jnp.where(mask, grad, jnp.zeros_like(grad))
                probs = jnp.exp(dot(key, query_one, 1, 1) - lse[pair, head : head + 1, rows])
                prob_grad = dot(value, grad_one, 1, 1)
                delta = jnp.sum(mixed[span], axis=0, keepdims=True)
                score_grad = (probs * (prob_grad - delta) * HEAD_DIM**-0.5).astype(bf16)
                dv_sum[...] += dot(probs.astype(bf16), grad_one)
                dk_sum[...] += dot(score_grad, query_one)
                pieces.append(dot(k_flip[span, :], score_grad))
            query_grad = jnp.concatenate(pieces, axis=0).T
            dqkv_v[rows, q_lanes] = query_grad.astype(bf16)
            return sums + jnp.sum(query_grad, axis=0, keepdims=True)

        sums = lax.fori_loop(0, length // rows_q, one_block, jnp.zeros((1, LANES), f32))
        dqkv_v[:, k_lanes] = (dk_sum[...] * HEAD_DIM**0.5).astype(bf16)
        dqkv_v[:, v_lanes] = dv_sum[...].astype(bf16)
        vec_v[4:5, lanes_at(group * head_cols + pair * LANES, LANES)] = sums
        vec_v[4:5, lanes_at(width + group * head_cols + pair * LANES, LANES)] = jnp.sum(
            dv_sum[...], axis=0, keepdims=True
        )
        for turn, calls in enumerate(hooks[:pairs]):

            @pl.when(pair == turn)
            def _():
                for call in calls:
                    call()

        return carry

    split = max(1, pairs // 2)
    width_a, width_b = split * LANES, (pairs - split) * LANES

    def weigh(ref, start, cols):
        for q in range(chips):
            block = pl.ds(q * 2 * shard, 2 * shard)
            if ranks > 1:
                ref[block, :] = jnp.zeros((2 * shard, ref.shape[1]), bf16)
            for part in range(3):
                value = dot(
                    hid_v[block, :],
                    dqkv_v[:, part * head_cols + start : part * head_cols + start + cols],
                )
                ref[block, lanes_at((at.rank * 3 + part) * cols, cols)] = value.astype(bf16)

    hooks = [
        [share2.add_chips],
        [share2.step, sharep.add_chips],
        [share1.relay, share2.step, sharep.step],
        [share1.add_chips, sharea.relay, share2.step, sharep.step],
    ]
    hooks[split - 1] += [lambda: weigh(ga_v, 0, width_a), sharea.spread]
    lax.fori_loop(0, pairs, one_pair, 0)
    for calls in hooks[pairs:]:
        for call in calls:
            call()

    def widen(s, carry):
        rows = rows_at(s * tokens, tokens)
        partial = dot(dqkv_v[rows, :], wq_v[...], 1, 1)
        normed, _ = norm_stats(img_v[rows, :].astype(f32))
        vec_v[2:3, :width] += jnp.sum(partial * normed, axis=0, keepdims=True)
        vec_v[3:4, :width] += jnp.sum(partial, axis=0, keepdims=True)
        near_rows = rows_at(s * half, half)

        @pl.when(at.core == 0)
        def _():
            keep_v[near_rows, :] = partial[:half]
            da_v[near_rows, :] = partial[half:].astype(bf16)

        @pl.when(at.core == 1)
        def _():
            keep_v[near_rows, :] = partial[half:]
            da_v[near_rows, :] = partial[:half].astype(bf16)

        return carry

    lax.fori_loop(0, seq_ways, widen, 0)
    near_rows = pl.ds(0, seq_ways * half)
    near_copy = copies.remote(da_v.at[near_rows, :], near_v, dp=other)
    share1.step()
    sharea.add_chips()
    share2.finish()
    sharep.step()

    weigh(gb_v, width_a, width_b)
    extra_at = ranks * 3 * width_b
    per_chip = width // chips
    for q in range(chips):
        rows = [vec_v[2:3, q * per_chip + i : q * per_chip + i + LANES] for i in range(0, per_chip, LANES)]
        rows += [vec_v[3:4, q * per_chip + i : q * per_chip + i + LANES] for i in range(0, per_chip, LANES)]
        rows += [
            vec_v[4:5, 2 * q * per_chip + i : 2 * q * per_chip + i + LANES]
            for i in range(0, 2 * per_chip, LANES)
        ]
        which = lax.broadcasted_iota(jnp.int32, (16, LANES), 0)
        extra = jnp.zeros((16, LANES), f32)
        for i, row in enumerate(rows):
            extra = jnp.where(which == i, row, extra)
        gb_v[pl.ds(q * 2 * shard + 16, 2 * shard - 16), extra_at : extra_at + LANES] = jnp.zeros(
            (2 * shard - 16, LANES), bf16
        )
        gb_v[pl.ds(q * 2 * shard, 16), extra_at : extra_at + LANES] = extra.astype(bf16)
    shareb.spread()

    near_copy.wait_recv()
    home_core = lax.div(at.item, items)
    home_item = lax.rem(at.item, items)
    home_jobs = []
    for s in range(seq_ways):
        rows = pl.ds(s * half, half)
        rgl_v[rows, :] = (keep_v[rows, :] + near_v[rows, :].astype(f32)).astype(bf16)
        mine = (at.seq == s) & (at.core == home_core)
        dst = home_out.at[
            rows_at(at.rank * own_rows + home_item * tokens + at.core * half, half), :
        ]
        far = pltpu.make_async_remote_copy(
            src_ref=rgl_v.at[rows, :],
            dst_ref=dst,
            send_sem=home_send.at[s],
            recv_sem=home_recv,
            device_id={"dp": at.chip * 2 + home_core, "seq": s},
            device_id_type=pl.DeviceIdType.MESH,
        )
        near = pltpu.make_async_copy(rgl_v.at[rows, :], dst, home_recv)
        pl.when(mine)(near.start)
        pl.when(jnp.logical_not(mine))(far.start)
        home_jobs.append((mine, far))

    theirs = rows_at((1 - at.core) * shard, shard)
    ours = rows_at(at.core * shard, shard)
    units = final1.shape[1] // chips

    def place_one(ref, rows, core):
        for q in range(chips):
            cols = pl.ds(q * units, units)
            o1_out[:, lanes_at((2 * q + core) * units, units)] = ref[rows, cols]

    def place_q(ref, rows, core, start, cols):
        for j in range(ranks):
            for part in range(3):
                lane = part * width + (j * 2 + core) * head_cols + start
                oq_out[:, lanes_at(lane, cols)] = ref[rows, pl.ds((j * 3 + part) * cols, cols)]

    copies.local(final2, o2_out)
    share1.step()
    sharea.step()
    sharep.finish()
    copies.local(finalp, op_out)
    share1.step()
    sharea.step()
    shareb.relay()
    share1.finish()
    swap1_copy = copies.remote(final1.at[theirs, :], swap1, dp=other)
    sharea.step()
    shareb.add_chips()
    place_one(final1, ours, at.core)
    sharea.finish()
    swapa_copy = copies.remote(finala.at[theirs, :], swapa, dp=other)
    place_q(finala, ours, at.core, 0, width_a)
    shareb.step()
    swap1_copy.wait_recv()
    place_one(swap1, pl.ds(0, shard), 1 - at.core)
    shareb.step()
    swapa_copy.wait_recv()
    place_q(swapa, pl.ds(0, shard), 1 - at.core, 0, width_a)
    shareb.finish()
    swapb_copy = copies.remote(finalb.at[theirs, :], swapb, dp=other)
    swapx_copy = copies.remote(finalb.at[pl.ds(0, 16), pl.ds(extra_at, LANES)], swapx, dp=other)
    place_q(finalb, ours, at.core, width_a, width_b)
    swapb_copy.wait_recv()
    place_q(swapb, pl.ds(0, shard), 1 - at.core, width_a, width_b)
    swapx_copy.wait_recv()
    ox_out[...] = finalb[0:16, extra_at : extra_at + LANES].astype(f32) + swapx[...].astype(f32)
    pltpu.make_async_copy(home_out, home_out, home_recv).wait()
    for mine, far in home_jobs:
        pl.when(jnp.logical_not(mine))(far.wait_send)
    copies.finish()


def backward(items, rgl, wp, g2, g1, gp, prj, heads, img, wq, small, lse):
    dp_ways, seq_ways = lax.axis_size("dp"), lax.axis_size("seq")
    chips = dp_ways // 2
    ranks = seq_ways // (2 * items)
    own_rows, width = rgl.shape
    shard = width // dp_ways
    length, head_cols = heads.shape
    tokens = own_rows // items
    half = tokens // 2
    unit_rows = g2.shape[0] // chips
    units_half = g1.shape[1]
    gp_rows, gp_cols = gp.shape
    block_p = gp_rows // dp_ways
    split = max(1, head_cols // LANES // 2) * LANES
    cols_a, cols_b = ranks * 3 * split, ranks * 3 * (head_cols - split) + LANES
    stage_rows = max(own_rows, seq_ways * half)
    any_spec = pl.BlockSpec(memory_space=pl.ANY)
    vmem_spec = pl.BlockSpec(memory_space=pltpu.VMEM)
    low = lambda *shape: pltpu.VMEM(shape, bf16)

    def share(rows, cols):
        return [
            low(4 if chips == 4 else chips - 1, rows, cols),
            low(rows, cols),
            low(rows - rows // seq_ways, cols),
            low(rows, cols),
        ]

    remotes = 96
    return pl.pallas_call(
        functools.partial(backward_kernel, items),
        in_specs=[any_spec] * 10 + [vmem_spec],
        out_specs=[any_spec] * 3 + [vmem_spec] * 3,
        out_shape=[
            jax.ShapeDtypeStruct((ranks * own_rows, width), bf16),
            jax.ShapeDtypeStruct((unit_rows, width), bf16),
            jax.ShapeDtypeStruct((block_p, gp_cols), bf16),
            jax.ShapeDtypeStruct((shard, 2 * units_half), bf16),
            jax.ShapeDtypeStruct((shard, 3 * width), bf16),
            jax.ShapeDtypeStruct((16, LANES), f32),
        ],
        scratch_shapes=[
            low(stage_rows, width),
            low(width, width),
            low(length, 3 * head_cols),
            low(length, head_cols),
            low(length, width),
            low(width, 3 * head_cols),
            pltpu.VMEM(small.shape, f32),
            low(stage_rows, width),
            low(length, head_cols),
            low(width, length),
            low(length, 3 * head_cols),
            pltpu.VMEM((seq_ways * half, width), f32),
            low(seq_ways * half, width),
            pltpu.VMEM((8, 2 * width), f32),
            low(LANES, length),
            pltpu.VMEM((length, LANES), f32),
            pltpu.VMEM((length, LANES), f32),
            *share(unit_rows, width),
            *share(2 * shard, units_half),
            low(gp_rows // 2, gp_cols),
            low(gp_rows // 2, gp_cols),
            *share(block_p, gp_cols),
            low(width, cols_a),
            *share(2 * shard, cols_a),
            low(width, cols_b),
            *share(2 * shard, cols_b),
            low(shard, units_half),
            low(shard, cols_a),
            low(shard, cols_b),
            low(16, LANES),
            pltpu.SemaphoreType.DMA((remotes,)),
            pltpu.SemaphoreType.DMA((remotes,)),
            pltpu.SemaphoreType.DMA((32,)),
            pltpu.SemaphoreType.DMA((2 * items * ranks,)),
            pltpu.SemaphoreType.DMA((seq_ways,)),
            pltpu.SemaphoreType.DMA((seq_ways,)),
            pltpu.SemaphoreType.DMA,
        ],
        compiler_params=pltpu.CompilerParams(
            collective_id=1, has_side_effects=True, vmem_limit_bytes=67043328
        ),
        name="backward",
    )(rgl, wp, g2, g1, gp, prj, heads, img, wq, small, lse)


def body(
    images,
    qkv_weight,
    qv_bias,
    proj_weight,
    proj_bias,
    ln1_gain,
    ln1_bias,
    ln2_gain,
    ln2_bias,
    fc1_weight,
    fc1_bias,
    fc2_weight,
    fc2_bias,
    cotangent,
):
    items, tokens, width = images.shape
    own_rows = items * tokens
    seq_ways, dp_ways = lax.axis_size("seq"), lax.axis_size("dp")
    chips = dp_ways // 2
    shard_rows = width // dp_ways
    column_items = 2 * items
    ranks = seq_ways // column_items
    groups = 2 * ranks
    head_cols = width // groups
    length = seq_ways * tokens
    half = tokens // 2
    dp_index, seq_index = lax.axis_index("dp"), lax.axis_index("seq")
    core, chip = dp_index % 2, dp_index // 2
    first_core = core == 0
    rank = seq_index % ranks
    group = rank * 2 + core
    same_core = [[2 * q + c for q in range(chips)] for c in range(2)]

    def swap(array):
        return lax.ppermute(array, "dp", [(i, i ^ 1) for i in range(dp_ways)])

    def by_core(own, other, axis):
        return jnp.where(
            first_core, jnp.stack([own, other], axis), jnp.stack([other, own], axis)
        )

    def pick(array, index, axis):
        return lax.dynamic_index_in_dim(array, index, axis, keepdims=False)

    def hop(array, bits):
        return lax.ppermute(array, "dp", [(i, i ^ (2 * bits)) for i in range(dp_ways)])

    def gather_chips(block):
        if chips != 4:
            return lax.all_gather(block, "dp", axis=0, axis_index_groups=same_core)
        gathered = jnp.zeros((4,) + block.shape, block.dtype)
        gathered = lax.dynamic_update_index_in_dim(gathered, block, chip, 0)
        for bits in (1, 2, 3):
            gathered = lax.dynamic_update_index_in_dim(gathered, hop(block, bits), chip ^ bits, 0)
        return gathered

    def scatter_chips(blocks):
        if chips != 4:
            return lax.psum_scatter(
                blocks, "dp", scatter_dimension=0, tiled=False, axis_index_groups=same_core
            )
        total = pick(blocks, chip, 0).astype(f32)
        for bits in (1, 2, 3):
            total = total + hop(pick(blocks, chip ^ bits, 0), bits).astype(f32)
        return total.astype(bf16)

    small_names = (qv_bias, proj_bias, ln1_gain, ln1_bias, ln2_gain, ln2_bias, fc1_bias, fc2_bias)
    small = jnp.concatenate([array.reshape(-1, shard_rows) for array in small_names]).astype(f32)
    small = jnp.pad(small, ((0, 16 - small.shape[0]), (0, LANES - shard_rows)))
    cotangent_own = cotangent.reshape(own_rows, width)
    (
        image_low,
        qkv_full,
        proj_full,
        fc1_half,
        fc2_half,
        cotangent_all,
        small,
        projected,
        attended,
        log_total,
        attended_rows,
        residual_first,
        hidden_second,
        pre_act,
        acts,
    ) = forward(
        items,
        images.reshape(own_rows, width),
        qkv_weight,
        proj_weight,
        fc1_weight,
        fc2_weight,
        cotangent_own,
        small,
    )
    small_all = small
    small = small.reshape(dp_ways, 16, LANES)
    smalls, at = [], 0
    for array in small_names:
        count = array.shape[0] // shard_rows
        smalls.append(small[:, at : at + count, :shard_rows].reshape(-1))
        at += count
    _, _, gain_first, _, gain_second, _, _, bias_two = smalls
    flat_rows = images.reshape(own_rows, width).astype(f32)
    normed_second, inv_second = norm_stats(residual_first)

    def meet(partial):
        parts = partial.reshape(2, own_rows, width)
        return pick(parts, core, 0) + swap(pick(parts, 1 - core, 0).astype(bf16)).astype(f32)

    output = residual_first + meet(dot(acts, fc2_half)) + bias_two

    pre_grad = dot(cotangent_all, fc2_half, 1, 1) * gelu_slope(pre_act)
    pre_grad_low = pre_grad.astype(bf16)
    grad_bias_one = jnp.sum(pre_grad, axis=0)
    grad_out = cotangent_own.astype(f32)
    grad_bias_two = jnp.sum(grad_out, axis=0)
    hidden_second_grad = meet(dot(pre_grad_low, fc1_half, 1, 1))
    grad_gain_second = jnp.sum(hidden_second_grad * normed_second, axis=0)
    grad_shift_second = jnp.sum(hidden_second_grad, axis=0)
    residual_grad = grad_out + norm_backward(
        hidden_second_grad, normed_second, inv_second, gain_second
    )
    residual_grad_low = residual_grad.astype(bf16)
    grad_proj_bias = jnp.sum(residual_grad, axis=0)
    grad_fc_two = dot(acts, cotangent_all, 0, 0).astype(bf16)
    grad_fc_one = dot(hidden_second, pre_grad_low, 0, 0).astype(bf16)
    grad_proj = dot(attended_rows, residual_grad_low, 0, 0).astype(bf16)

    def shares(vector):
        return vector.reshape(dp_ways, -1)

    one_parts = grad_bias_one.reshape(chips, 1, -1)
    one_all = jnp.where(
        jnp.arange(2)[None, :, None] == core, jnp.broadcast_to(one_parts, (chips, 2, one_parts.shape[2])), 0.0
    )
    block_rows = -(-shard_rows // (16 * seq_ways)) * 16 * seq_ways

    def by_owner(array):
        array = array.reshape((chips, 2) + array.shape[1:])
        return jnp.moveaxis(array, 1, 0)

    extra = jnp.concatenate(
        [
            shares(grad_proj_bias),
            shares(grad_gain_second),
            shares(grad_shift_second),
            shares(grad_bias_two),
            shares(one_all),
        ],
        axis=1,
    )
    extra = extra.reshape(dp_ways, -1, LANES).astype(bf16)
    extra_rows = extra.shape[1]
    extra = jnp.pad(extra, ((0, 0), (0, shard_rows - extra_rows), (0, 0)))
    blocks = jnp.concatenate([grad_proj.reshape(dp_ways, shard_rows, width), extra], axis=2)
    blocks = jnp.pad(blocks, ((0, 0), (0, block_rows - shard_rows), (0, 0)))
    blocks = by_owner(blocks).reshape(dp_ways * block_rows, width + LANES)

    home, share_two, share_proj, out_one, out_qkv, first_sums = backward(
        items,
        residual_grad_low,
        proj_full,
        grad_fc_two,
        grad_fc_one,
        blocks,
        projected,
        attended,
        image_low,
        qkv_full,
        small_all,
        log_total,
    )
    home = home.reshape(ranks, own_rows, width).astype(f32)
    hidden_first_grad = jnp.sum(home, axis=0) if ranks > 1 else home[0]
    normed_first, inv_first = norm_stats(flat_rows)
    image_grad = residual_grad + norm_backward(
        hidden_first_grad, normed_first, inv_first, gain_first
    )
    per_chip = 2 * shard_rows
    first_sums = first_sums.reshape(-1)
    out_gain_first = pick(first_sums[:per_chip].reshape(2, -1), core, 0)
    out_shift_first = pick(first_sums[per_chip : 2 * per_chip].reshape(2, -1), core, 0)
    out_qv = pick(first_sums[2 * per_chip : 4 * per_chip].reshape(2, -1), core, 0)
    last = share_proj[:extra_rows, width:].reshape(-1).astype(f32)
    out_smalls, at = [], 0
    for size in (shard_rows, shard_rows, shard_rows, shard_rows, 4 * shard_rows):
        out_smalls.append(last[at : at + size])
        at += size
    return (
        output.reshape(images.shape),
        image_grad.reshape(images.shape),
        out_qkv.astype(f32),
        out_qv,
        share_proj[:shard_rows, :width].astype(f32),
        out_smalls[0],
        out_gain_first,
        out_shift_first,
        out_smalls[1],
        out_smalls[2],
        out_one.astype(f32),
        out_smalls[4],
        share_two.astype(f32),
        out_smalls[3],
    )


def solution(mesh):
    rows, cols, flat = P("dp", "seq", None), P("dp", None), P("dp")
    in_specs = (rows, cols, flat, cols, flat, flat, flat, flat, flat, cols, flat, cols, flat, rows)
    out_specs = (rows, rows, cols, flat, cols, flat, flat, flat, flat, flat, cols, flat, cols, flat)
    return jax.shard_map(body, mesh=mesh, in_specs=in_specs, out_specs=out_specs, check_vma=False)
```
